16 devices in a mesh: lev: 2 (over y, z), w: 8 (over x, core).
Axes of the slice: x: 4, y: 2, z: 1, core: 2. Of those that a mesh axis runs over, the one named last changes fastest.
The devices are a block of a 4x4x8 slice.
Arguments:
- coef: float32 [160, 2, 256, 160], P('w', None, 'lev'), parts along dimension 2
- legendre: float32 [160, 160, 160], replicated
- gauss_weight: float32 [160], replicated
Outputs:
- output 1: float32 [256, 160, 320], P('lev', 'w'), parts along dimension 0
- output 2: float32 [160, 2, 256, 160], P('w', None, 'lev'), parts along dimension 2
There are 2 independent parts. The reference program is written for one: setup_inputs(seed, part) draws one part's arguments, and reference() takes and returns one part's arrays. A program takes and returns all parts, laid end to end along the dimension named above; an argument that names none is the same for every part.
All inputs are finite; a program needn't handle non-finite values.
Results may differ from the reference program's by a relative error of at most 0.001.
Values sent between devices are 32-bit elements.
A program may use at most 768 MiB of HBM per device.

```python
import jax
import jax.numpy as jnp
from jax import lax

WAVE_NUM = 160
LAT_ROWS = 160
LEVELS = 128


def setup_inputs(seed: int = 0, part: int = 0) -> dict:
    base_key = jax.random.key(seed)
    key_coef = jax.random.fold_in(jax.random.fold_in(base_key, 1), part)
    key_leg = jax.random.fold_in(base_key, 2)
    key_wt = jax.random.fold_in(base_key, 3)
    wave_idx = jnp.arange(WAVE_NUM)
    row_m = wave_idx[:, None].astype(jnp.float32)
    col_l = wave_idx[None, :].astype(jnp.float32)
    live_mask = wave_idx[None, :] >= wave_idx[:, None]
    amplitude = jnp.sqrt(WAVE_NUM / ((WAVE_NUM - row_m) * (1.0 + (col_l - row_m) / WAVE_NUM)))
    coef_mask = jnp.stack([live_mask, live_mask & (wave_idx[:, None] > 0)], axis=1)[:, :, None, :]
    draw_coef = jax.random.normal(key_coef, (WAVE_NUM, 2, LEVELS, WAVE_NUM), jnp.float32)
    coef = jnp.where(coef_mask, draw_coef * amplitude[:, None, None, :], 0.0)
    draw_leg = jax.random.normal(key_leg, (WAVE_NUM, WAVE_NUM, LAT_ROWS), jnp.float32)
    legendre = jnp.where(live_mask[:, :, None], draw_leg, 0.0)
    gauss_weight = jax.random.uniform(key_wt, (LAT_ROWS,), jnp.float32, 0.5, 1.5) / LAT_ROWS
    return {'coef': coef, 'legendre': legendre, 'gauss_weight': gauss_weight}


def reference(coef, legendre, gauss_weight):
    lon_pts = 2 * WAVE_NUM
    splits = 8
    lat_blk = LAT_ROWS // splits

    def lat_step(spec_acc, blk_idx):
        lat_start = blk_idx * lat_blk
        leg_blk = lax.dynamic_slice_in_dim(legendre, lat_start, lat_blk, axis=2).astype(jnp.float32)
        wt_blk = lax.dynamic_slice_in_dim(gauss_weight, lat_start, lat_blk, axis=0)
        fourier = jnp.einsum('mrkl,mlj->mrkj', coef.astype(jnp.float32), leg_blk)
        spec = lax.complex(fourier[:, 0], fourier[:, 1])
        grid_blk = jnp.fft.irfft(spec, n=lon_pts, axis=0)
        square_hat = jnp.fft.rfft(grid_blk * grid_blk, axis=0)[:WAVE_NUM] * wt_blk[None, None, :]
        re_im = jnp.stack([jnp.real(square_hat), jnp.imag(square_hat)], axis=1)
        spec_acc = spec_acc + jnp.einsum('mrkj,mlj->mrkl', re_im, leg_blk)
        return spec_acc, jnp.transpose(grid_blk, (1, 2, 0))

    spec_out, grid_parts = lax.scan(lat_step, jnp.zeros(coef.shape, jnp.float32), jnp.arange(splits))
    grid = jnp.transpose(grid_parts, (1, 0, 2, 3)).reshape(LEVELS, LAT_ROWS, lon_pts)
    return grid, spec_out
```

```python
import functools

import jax
import jax.numpy as jnp
import ml_dtypes
import numpy as np
from jax import lax
from jax.experimental import pallas as pl
from jax.experimental.pallas import tpu as pltpu
from jax.sharding import PartitionSpec as P

MESH = pl.DeviceIdType.MESH
F32, BF16 = jnp.float32, jnp.bfloat16
LANES = 128
SUB = 8
QUAD = 4
GROUPS = 4


def split_np(mat):
    hi = mat.astype(np.float32).astype(ml_dtypes.bfloat16)
    lo = (mat - hi.astype(np.float64)).astype(np.float32).astype(ml_dtypes.bfloat16)
    return hi, lo


def fourier_matrices(waves):
    lon = 2 * waves
    m = np.arange(waves)[:, None]
    n = np.arange(lon)[None, :]
    ang = 2.0 * np.pi * ((m * n) % lon) / lon
    fwd = np.concatenate([np.cos(ang), -np.sin(ang)], axis=0)
    scale = np.where(np.arange(waves) == 0, 1.0, 2.0) / lon
    inv = (fwd * np.tile(scale, 2)[:, None]).T
    out = []
    for mat in (inv, fwd):
        hi, lo = split_np(mat)
        out.append(np.concatenate([hi, hi, lo], axis=1))
    return out


def split(x):
    hi = x.astype(BF16)
    lo = (x - hi.astype(F32)).astype(BF16)
    return hi, lo


def dot(a, b, dims=((1,), (0,))):
    return lax.dot_general(a, b, (dims, ((), ())), preferred_element_type=F32)


def kernel(dims, coef_hbm, leg_hbm, inv_hbm, fwd_hbm, wt_ref, grid_hbm, spec_hbm,
           coef, leg, inv, fwd, send_a, recv_a, send_b, recv_b, grid, spec,
           load_sem, mat_sem, send_sem_a, recv_sem_a, send_sem_b, recv_sem_b, last_sem, out_sem, grid_sem):
    group, wave_loc, levels, degs, lat_loc, lat_pad, waves, lon = dims
    chunks = lat_loc // QUAD
    planes = -(-lon // LANES)
    per_group = wave_loc // GROUPS
    msg = wave_loc * SUB
    part = per_group * SUB
    me = lax.axis_index('w')

    barrier = pltpu.get_barrier_semaphore()
    for off in range(1, group):
        pl.semaphore_signal(barrier, inc=1, device_id={'w': lax.rem(me + off, group)}, device_id_type=MESH)

    loads = []
    for g in range(GROUPS):
        own = pl.ds(g * per_group, per_group)
        first = pltpu.make_async_copy(coef_hbm.at[own], coef.at[own], load_sem.at[0, g])
        second = pltpu.make_async_copy(leg_hbm.at[pl.ds(me * wave_loc + g * per_group, per_group)], leg.at[own], load_sem.at[1, g])
        first.start()
        second.start()
        loads.append((first, second))
    mats = [pltpu.make_async_copy(inv_hbm, inv, mat_sem.at[0]), pltpu.make_async_copy(fwd_hbm, fwd, mat_sem.at[1])]
    for copy in mats:
        copy.start()

    low = lax.broadcasted_iota(jnp.int32, (SUB, levels), 0) < QUAD

    def rows(start, size):
        return pl.ds(pl.multiple_of(start, SUB), size)

    def copy_a(off, c, start, size):
        dst = lax.rem(me + off, group)
        return pltpu.make_async_remote_copy(
            src_ref=send_a.at[rows((dst * chunks + c) * msg + start, size)],
            dst_ref=recv_a.at[rows((c * group + me) * msg + start, size)],
            send_sem=send_sem_a, recv_sem=recv_sem_a.at[c], device_id={'w': dst}, device_id_type=MESH)

    def copy_b(off, c, start, size, sem):
        dst = lax.rem(me + off, group)
        return pltpu.make_async_remote_copy(
            src_ref=send_b.at[rows((c * group + dst) * msg + start, size)],
            dst_ref=recv_b.at[rows((c * group + me) * msg + start, size)],
            send_sem=send_sem_b, recv_sem=sem, device_id={'w': dst}, device_id_type=MESH)

    order = [group // 2, 2, group - 2, group // 2 + 1, 3, group - 1, 1]
    order = order if sorted(order) == list(range(1, group)) else list(range(1, group))

    for g in range(GROUPS):
        for copy in loads[g]:
            copy.wait()

        def legendre_body(i, carry):
            m = g * per_group + i
            leg_hi, leg_lo = split(jnp.transpose(leg[m]))
            c_hi, c_lo = split(coef[m].reshape(2 * levels, degs))
            nt = ((1,), (1,))
            f = dot(leg_hi, c_hi, nt) + dot(leg_lo, c_hi, nt) + dot(leg_hi, c_lo, nt)
            for t in range(group * lat_loc // SUB):
                re = f[t * SUB:(t + 1) * SUB, :levels]
                im = f[t * SUB:(t + 1) * SUB, levels:]
                send_a[rows((2 * t * wave_loc + m) * SUB, SUB), :] = jnp.where(low, re, pltpu.roll(im, QUAD, 0))
                send_a[rows(((2 * t + 1) * wave_loc + m) * SUB, SUB), :] = jnp.where(low, pltpu.roll(re, QUAD, 0), im)
            return carry

        lax.fori_loop(0, per_group, legendre_body, 0)
        if g == 0:
            pl.semaphore_wait(barrier, group - 1)
        for off in order:
            copy_a(off, 0, g * part, part).start()

    @pl.loop(1, chunks)
    def _(c):
        for off in order:
            copy_a(off, c, 0, msg).start()

    @pl.loop(0, chunks)
    def _(c):
        recv_a[rows((c * group + me) * msg, msg), :] = send_a[rows((me * chunks + c) * msg, msg), :]

    for copy in mats:
        copy.wait()

    @pl.loop(0, chunks)
    def _(c):
        landed = recv_a.at[pl.ds(0, (group - 1) * msg)]
        pltpu.make_async_copy(landed, landed, recv_sem_a.at[c]).wait()

        @pl.loop(0, QUAD // 2)
        def _(pair):
            halves = []
            for u in range(2):
                row = c * (group * msg) + 2 * pair + u
                re = recv_a[pl.ds(row, waves, stride=SUB), :]
                im = recv_a[pl.ds(row + QUAD, waves, stride=SUB), :]
                halves.append(jnp.concatenate([re, im], axis=0))
            f_hi, f_lo = split(jnp.concatenate(halves, axis=1))
            g_val = dot(inv[...], jnp.concatenate([f_hi, f_lo, f_hi], axis=0))
            for u in range(2):
                j = c * QUAD + 2 * pair + u
                for p in range(planes):
                    piece = g_val[p * LANES:min((p + 1) * LANES, lon), u * levels:(u + 1) * levels]
                    if piece.shape[0] < LANES:
                        piece = jnp.concatenate([piece, jnp.zeros((LANES - piece.shape[0], levels), F32)], axis=0)
                    grid[pl.ds(p * levels * lat_pad + j, levels, stride=lat_pad), :] = jnp.transpose(piece)
            q_hi, q_lo = split(g_val * g_val)
            h = dot(fwd[...], jnp.concatenate([q_hi, q_lo, q_hi], axis=0))
            for u in range(2):
                row = c * (group * msg) + 2 * pair + u
                hw = h[:, u * levels:(u + 1) * levels] * wt_ref[me * lat_loc + c * QUAD + 2 * pair + u]
                send_b[pl.ds(row, waves, stride=SUB), :] = hw[:waves]
                send_b[pl.ds(row + QUAD, waves, stride=SUB), :] = hw[waves:]

        @pl.when(c < chunks - 1)
        def _():
            for off in order:
                copy_b(off, c, 0, msg, recv_sem_b).start()

        @pl.when(c == chunks - 1)
        def _():
            for g in range(GROUPS):
                for off in order:
                    copy_b(off, c, g * part, part, last_sem.at[g]).start()

        recv_b[rows((c * group + me) * msg, msg), :] = send_b[rows((c * group + me) * msg, msg), :]

    grid_out = []
    for p in range(planes):
        copy = pltpu.make_async_copy(grid.at[pl.ds(p * levels * lat_pad, levels * lat_pad)], grid_hbm.at[:, pl.ds(p * LANES, LANES)], grid_sem.at[p])
        copy.start()
        grid_out.append(copy)

    landed = recv_b.at[pl.ds(0, (chunks - 1) * (group - 1) * msg)]
    pltpu.make_async_copy(landed, landed, recv_sem_b).wait()
    outs = []
    for g in range(GROUPS):
        landed = recv_b.at[pl.ds(0, (group - 1) * part)]
        pltpu.make_async_copy(landed, landed, last_sem.at[g]).wait()

        def back_body(i, carry):
            m = g * per_group + i
            re, im = [], []
            for t in range(group * lat_loc // SUB):
                tiles = []
                for q in (2 * t, 2 * t + 1):
                    s, c = divmod(q, chunks)
                    tiles.append(recv_b[rows(((c * group + s) * wave_loc + m) * SUB, SUB), :])
                a, b = tiles
                re.append(jnp.where(low, a, pltpu.roll(b, QUAD, 0)))
                im.append(jnp.where(low, pltpu.roll(a, QUAD, 0), b))
            h_hi, h_lo = split(jnp.concatenate([jnp.concatenate(re, axis=0), jnp.concatenate(im, axis=0)], axis=1))
            leg_hi, leg_lo = split(leg[m])
            s_val = dot(leg_hi, h_hi) + dot(leg_lo, h_hi) + dot(leg_hi, h_lo)
            spec[m] = jnp.transpose(s_val).reshape(2, levels, degs)
            return carry

        lax.fori_loop(0, per_group, back_body, 0)
        own = pl.ds(g * per_group, per_group)
        copy = pltpu.make_async_copy(spec.at[own], spec_hbm.at[own], out_sem.at[g])
        copy.start()
        outs.append(copy)

    for copy in outs:
        copy.wait()
    for copy in grid_out:
        copy.wait()
    sent = send_a.at[pl.ds(0, (group - 1) * chunks * msg)]
    pltpu.make_async_copy(sent, sent, send_sem_a).wait()
    pltpu.make_async_copy(sent, sent, send_sem_b).wait()


def solution(mesh):
    group = mesh.shape['w']

    def per_device(coef, legendre, gauss_weight):
        wave_loc, _, levels, degs = coef.shape
        waves = wave_loc * group
        lon = 2 * waves
        lat_loc = legendre.shape[2] // group
        lat_pad = -(-lat_loc // SUB) * SUB
        inv, fwd = (jnp.asarray(x) for x in fourier_matrices(waves))
        planes = -(-lon // LANES)
        total = group * lat_loc // QUAD * wave_loc * SUB
        dims = (group, wave_loc, levels, degs, lat_loc, lat_pad, waves, lon)
        hbm = pl.BlockSpec(memory_space=pl.ANY)
        dma = pltpu.SemaphoreType.DMA
        grid, spec = pl.pallas_call(
            functools.partial(kernel, dims),
            out_shape=(jax.ShapeDtypeStruct((levels * lat_pad, planes * LANES), F32), jax.ShapeDtypeStruct(coef.shape, F32)),
            in_specs=[hbm, hbm, hbm, hbm, pl.BlockSpec(memory_space=pltpu.SMEM)],
            out_specs=(hbm, hbm),
            scratch_shapes=[
                pltpu.VMEM(coef.shape, F32),
                pltpu.VMEM((wave_loc, degs, legendre.shape[2]), F32),
                pltpu.VMEM(inv.shape, BF16),
                pltpu.VMEM(fwd.shape, BF16),
                pltpu.VMEM((total, levels), F32),
                pltpu.VMEM((total, levels), F32),
                pltpu.VMEM((total, levels), F32),
                pltpu.VMEM((total, levels), F32),
                pltpu.VMEM((planes * levels * lat_pad, LANES), F32),
                pltpu.VMEM(coef.shape, F32),
                dma((2, GROUPS)), dma((2,)), dma, dma((lat_loc // QUAD,)), dma, dma, dma((GROUPS,)), dma((GROUPS,)), dma((planes,)),
            ],
            compiler_params=pltpu.CompilerParams(collective_id=0, has_side_effects=True, vmem_limit_bytes=56 * 2**20),
            name='transform_pair',
        )(coef, legendre, inv, fwd, gauss_weight)
        return grid.reshape(levels, lat_pad, planes * LANES)[:, :lat_loc, :lon], spec

    return jax.shard_map(per_device, mesh=mesh, in_specs=(P('w', None, 'lev', None), P(None, None, None), P(None)), out_specs=(P('lev', 'w', None), P('w', None, 'lev', None)), check_vma=False)
```

```python
import functools

import jax
import jax.numpy as jnp
import ml_dtypes
import numpy as np
from jax import lax
from jax.experimental import pallas as pl
from jax.experimental.pallas import tpu as pltpu
from jax.sharding import PartitionSpec as P

MESH = pl.DeviceIdType.MESH
F32, BF16 = jnp.float32, jnp.bfloat16
SUB = 8
QUAD = 4
GROUPS = 4


def split_np(mat):
    hi = mat.astype(np.float32).astype(ml_dtypes.bfloat16)
    lo = (mat - hi.astype(np.float64)).astype(np.float32).astype(ml_dtypes.bfloat16)
    return hi, lo


def fourier_matrices(waves):
    lon = 2 * waves
    m = np.arange(waves)[:, None]
    n = np.arange(lon)[None, :]
    ang = 2.0 * np.pi * ((m * n) % lon) / lon
    fwd = np.concatenate([np.cos(ang), -np.sin(ang)], axis=0)
    scale = np.where(np.arange(waves) == 0, 1.0, 2.0) / lon
    inv = (fwd * np.tile(scale, 2)[:, None]).T
    out = []
    for mat in (inv, fwd):
        hi, lo = split_np(mat)
        out.append(np.concatenate([hi, hi, lo], axis=1))
    return out


def split(x):
    hi = x.astype(BF16)
    lo = (x - hi.astype(F32)).astype(BF16)
    return hi, lo


def dot(a, b, dims=((1,), (0,))):
    return lax.dot_general(a, b, (dims, ((), ())), preferred_element_type=F32)


def kernel(dims, coef_hbm, leg_hbm, inv_hbm, fwd_hbm, wt_ref, grid_hbm, spec_hbm,
           coef, leg, inv, fwd, send_a, recv_a, send_b, recv_b, grid, spec,
           load_sem, mat_sem, send_sem_a, recv_sem_a, send_sem_b, recv_sem_b, last_sem, out_sem, grid_sem):
    group, wave_loc, levels, degs, lat_loc, waves, lon = dims
    chunks = lat_loc // QUAD
    per_group = wave_loc // GROUPS
    msg = wave_loc * SUB
    part = per_group * SUB
    me = lax.axis_index('w')

    barrier = pltpu.get_barrier_semaphore()
    for off in range(1, group):
        pl.semaphore_signal(barrier, inc=1, device_id={'w': lax.rem(me + off, group)}, device_id_type=MESH)

    loads = []
    for g in range(GROUPS):
        own = pl.ds(g * per_group, per_group)
        first = pltpu.make_async_copy(coef_hbm.at[own], coef.at[own], load_sem.at[0, g])
        second = pltpu.make_async_copy(leg_hbm.at[pl.ds(me * wave_loc + g * per_group, per_group)], leg.at[own], load_sem.at[1, g])
        first.start()
        second.start()
        loads.append((first, second))
    mats = [pltpu.make_async_copy(inv_hbm, inv, mat_sem.at[0]), pltpu.make_async_copy(fwd_hbm, fwd, mat_sem.at[1])]
    for copy in mats:
        copy.start()

    low = lax.broadcasted_iota(jnp.int32, (SUB, levels), 0) < QUAD

    def rows(start, size):
        return pl.ds(pl.multiple_of(start, SUB), size)

    def copy_a(off, c, start, size):
        dst = lax.rem(me + off, group)
        return pltpu.make_async_remote_copy(
            src_ref=send_a.at[rows((dst * chunks + c) * msg + start, size)],
            dst_ref=recv_a.at[rows((c * group + me) * msg + start, size)],
            send_sem=send_sem_a, recv_sem=recv_sem_a.at[c], device_id={'w': dst}, device_id_type=MESH)

    def copy_b(off, c, start, size, sem):
        dst = lax.rem(me + off, group)
        return pltpu.make_async_remote_copy(
            src_ref=send_b.at[rows((c * group + dst) * msg + start, size)],
            dst_ref=recv_b.at[rows((c * group + me) * msg + start, size)],
            send_sem=send_sem_b, recv_sem=sem, device_id={'w': dst}, device_id_type=MESH)

    order = [group // 2, 2, group - 2, group // 2 + 1, 3, group - 1, 1]
    order = order if sorted(order) == list(range(1, group)) else list(range(1, group))

    for g in range(GROUPS):
        for copy in loads[g]:
            copy.wait()

        def legendre_body(i, carry):
            m = g * per_group + i
            leg_hi, leg_lo = split(jnp.transpose(leg[m]))
            c_hi, c_lo = split(jnp.concatenate([coef[m, 0], coef[m, 1]], axis=1))
            f = dot(leg_hi, c_hi) + dot(leg_lo, c_hi) + dot(leg_hi, c_lo)
            for t in range(group * lat_loc // SUB):
                re = f[t * SUB:(t + 1) * SUB, :levels]
                im = f[t * SUB:(t + 1) * SUB, levels:]
                send_a[rows((2 * t * wave_loc + m) * SUB, SUB), :] = jnp.where(low, re, pltpu.roll(im, QUAD, 0))
                send_a[rows(((2 * t + 1) * wave_loc + m) * SUB, SUB), :] = jnp.where(low, pltpu.roll(re, QUAD, 0), im)
            return carry

        lax.fori_loop(0, per_group, legendre_body, 0)
        if g == 0:
            pl.semaphore_wait(barrier, group - 1)
        for off in order:
            copy_a(off, 0, g * part, part).start()

    @pl.loop(1, chunks)
    def _(c):
        for off in order:
            copy_a(off, c, 0, msg).start()

    @pl.loop(0, chunks)
    def _(c):
        recv_a[rows((c * group + me) * msg, msg), :] = send_a[rows((me * chunks + c) * msg, msg), :]

    for copy in mats:
        copy.wait()

    @pl.loop(0, chunks)
    def _(c):
        landed = recv_a.at[pl.ds(0, (group - 1) * msg)]
        pltpu.make_async_copy(landed, landed, recv_sem_a.at[c]).wait()

        @pl.loop(0, QUAD // 2)
        def _(pair):
            halves = []
            for u in range(2):
                row = c * (group * msg) + 2 * pair + u
                re = recv_a[pl.ds(row, waves, stride=SUB), :]
                im = recv_a[pl.ds(row + QUAD, waves, stride=SUB), :]
                halves.append(jnp.concatenate([re, im], axis=0))
            f_hi, f_lo = split(jnp.concatenate(halves, axis=1))
            g_val = dot(inv[...], jnp.concatenate([f_hi, f_lo, f_hi], axis=0))
            for u in range(2):
                grid[c * QUAD + 2 * pair + u] = g_val[:, u * levels:(u + 1) * levels]
            q_hi, q_lo = split(g_val * g_val)
            h = dot(fwd[...], jnp.concatenate([q_hi, q_lo, q_hi], axis=0))
            for u in range(2):
                row = c * (group * msg) + 2 * pair + u
                hw = h[:, u * levels:(u + 1) * levels] * wt_ref[me * lat_loc + c * QUAD + 2 * pair + u]
                send_b[pl.ds(row, waves, stride=SUB), :] = hw[:waves]
                send_b[pl.ds(row + QUAD, waves, stride=SUB), :] = hw[waves:]

        @pl.when(c < chunks - 1)
        def _():
            for off in order:
                copy_b(off, c, 0, msg, recv_sem_b).start()

        @pl.when(c == chunks - 1)
        def _():
            for g in range(GROUPS):
                for off in order:
                    copy_b(off, c, g * part, part, last_sem.at[g]).start()

        lats = pl.ds(c * QUAD, QUAD)
        pltpu.make_async_copy(grid.at[lats], grid_hbm.at[lats], grid_sem).start()
        recv_b[rows((c * group + me) * msg, msg), :] = send_b[rows((c * group + me) * msg, msg), :]

    landed = recv_b.at[pl.ds(0, (chunks - 1) * (group - 1) * msg)]
    pltpu.make_async_copy(landed, landed, recv_sem_b).wait()
    outs = []
    for g in range(GROUPS):
        landed = recv_b.at[pl.ds(0, (group - 1) * part)]
        pltpu.make_async_copy(landed, landed, last_sem.at[g]).wait()

        def back_body(i, carry):
            m = g * per_group + i
            re, im = [], []
            for t in range(group * lat_loc // SUB):
                tiles = []
                for q in (2 * t, 2 * t + 1):
                    s, c = divmod(q, chunks)
                    tiles.append(recv_b[rows(((c * group + s) * wave_loc + m) * SUB, SUB), :])
                a, b = tiles
                re.append(jnp.where(low, a, pltpu.roll(b, QUAD, 0)))
                im.append(jnp.where(low, pltpu.roll(a, QUAD, 0), b))
            h_hi, h_lo = split(jnp.concatenate([jnp.concatenate(re, axis=0), jnp.concatenate(im, axis=0)], axis=1))
            leg_hi, leg_lo = split(leg[m])
            s_val = dot(leg_hi, h_hi) + dot(leg_lo, h_hi) + dot(leg_hi, h_lo)
            spec[m, 0] = s_val[:, :levels]
            spec[m, 1] = s_val[:, levels:]
            return carry

        lax.fori_loop(0, per_group, back_body, 0)
        own = pl.ds(g * per_group, per_group)
        copy = pltpu.make_async_copy(spec.at[own], spec_hbm.at[own], out_sem.at[g])
        copy.start()
        outs.append(copy)

    for copy in outs:
        copy.wait()
    pltpu.make_async_copy(grid, grid_hbm, grid_sem).wait()
    sent = send_a.at[pl.ds(0, (group - 1) * chunks * msg)]
    pltpu.make_async_copy(sent, sent, send_sem_a).wait()
    pltpu.make_async_copy(sent, sent, send_sem_b).wait()


def solution(mesh):
    group = mesh.shape['w']

    def per_device(coef, legendre, gauss_weight):
        wave_loc, _, levels, degs = coef.shape
        waves = wave_loc * group
        lon = 2 * waves
        lat_loc = legendre.shape[2] // group
        coef_t = jnp.transpose(coef, (0, 1, 3, 2))
        inv, fwd = (jnp.asarray(x) for x in fourier_matrices(waves))
        total = group * lat_loc // QUAD * wave_loc * SUB
        dims = (group, wave_loc, levels, degs, lat_loc, waves, lon)
        hbm = pl.BlockSpec(memory_space=pl.ANY)
        dma = pltpu.SemaphoreType.DMA
        grid, spec = pl.pallas_call(
            functools.partial(kernel, dims),
            out_shape=(jax.ShapeDtypeStruct((lat_loc, lon, levels), F32), jax.ShapeDtypeStruct(coef_t.shape, F32)),
            in_specs=[hbm, hbm, hbm, hbm, pl.BlockSpec(memory_space=pltpu.SMEM)],
            out_specs=(hbm, hbm),
            scratch_shapes=[
                pltpu.VMEM(coef_t.shape, F32),
                pltpu.VMEM((wave_loc, degs, legendre.shape[2]), F32),
                pltpu.VMEM(inv.shape, BF16),
                pltpu.VMEM(fwd.shape, BF16),
                pltpu.VMEM((total, levels), F32),
                pltpu.VMEM((total, levels), F32),
                pltpu.VMEM((total, levels), F32),
                pltpu.VMEM((total, levels), F32),
                pltpu.VMEM((lat_loc, lon, levels), F32),
                pltpu.VMEM(coef_t.shape, F32),
                dma((2, GROUPS)), dma((2,)), dma, dma((lat_loc // QUAD,)), dma, dma, dma((GROUPS,)), dma((GROUPS,)), dma,
            ],
            compiler_params=pltpu.CompilerParams(collective_id=0, has_side_effects=True, vmem_limit_bytes=56 * 2**20),
            name='transform_pair',
        )(coef_t, legendre, inv, fwd, gauss_weight)
        return jnp.transpose(grid, (2, 0, 1)), jnp.transpose(spec, (0, 1, 3, 2))

    return jax.shard_map(per_device, mesh=mesh, in_specs=(P('w', None, 'lev', None), P(None, None, None), P(None)), out_specs=(P('lev', 'w', None), P('w', None, 'lev', None)), check_vma=False)
```

```python
import functools

import jax
import jax.numpy as jnp
import ml_dtypes
import numpy as np
from jax import lax
from jax.experimental import pallas as pl
from jax.experimental.pallas import tpu as pltpu
from jax.sharding import PartitionSpec as P

MESH = pl.DeviceIdType.MESH
F32, BF16 = jnp.float32, jnp.bfloat16
SUB = 8
QUAD = 4
GROUPS = 4


def split_np(mat):
    hi = mat.astype(np.float32).astype(ml_dtypes.bfloat16)
    lo = (mat - hi.astype(np.float64)).astype(np.float32).astype(ml_dtypes.bfloat16)
    return hi, lo


def fourier_matrices(waves):
    lon = 2 * waves
    m = np.arange(waves)[:, None]
    n = np.arange(lon)[None, :]
    ang = 2.0 * np.pi * ((m * n) % lon) / lon
    fwd = np.concatenate([np.cos(ang), -np.sin(ang)], axis=0)
    scale = np.where(np.arange(waves) == 0, 1.0, 2.0) / lon
    inv = (fwd * np.tile(scale, 2)[:, None]).T
    out = []
    for mat in (inv, fwd):
        hi, lo = split_np(mat)
        out.append(np.concatenate([hi, hi, lo], axis=1))
    return out


def split(x):
    hi = x.astype(BF16)
    lo = (x - hi.astype(F32)).astype(BF16)
    return hi, lo


def dot(a, b, dims=((1,), (0,))):
    return lax.dot_general(a, b, (dims, ((), ())), preferred_element_type=F32)


def kernel(dims, coef_hbm, leg_hbm, inv_hbm, fwd_hbm, wt_ref, grid, spec,
           coef, leg, inv, fwd, send_a, recv_a, send_b, recv_b,
           load_sem, mat_sem, send_sem_a, recv_sem_a, send_sem_b, recv_sem_b, last_sem):
    group, wave_loc, levels, degs, lat_loc, waves, lon = dims
    chunks = lat_loc // QUAD
    per_group = wave_loc // GROUPS
    msg = wave_loc * SUB
    part = per_group * SUB
    me = lax.axis_index('w')

    barrier = pltpu.get_barrier_semaphore()
    for off in range(1, group):
        pl.semaphore_signal(barrier, inc=1, device_id={'w': lax.rem(me + off, group)}, device_id_type=MESH)

    loads = []
    for g in range(GROUPS):
        own = pl.ds(g * per_group, per_group)
        first = pltpu.make_async_copy(coef_hbm.at[own], coef.at[own], load_sem.at[0, g])
        second = pltpu.make_async_copy(leg_hbm.at[pl.ds(me * wave_loc + g * per_group, per_group)], leg.at[own], load_sem.at[1, g])
        first.start()
        second.start()
        loads.append((first, second))
    mats = [pltpu.make_async_copy(inv_hbm, inv, mat_sem.at[0]), pltpu.make_async_copy(fwd_hbm, fwd, mat_sem.at[1])]
    for copy in mats:
        copy.start()

    low = lax.broadcasted_iota(jnp.int32, (SUB, levels), 0) < QUAD

    def rows(start, size):
        return pl.ds(pl.multiple_of(start, SUB), size)

    def copy_a(off, c, start, size):
        dst = lax.rem(me + off, group)
        return pltpu.make_async_remote_copy(
            src_ref=send_a.at[rows((dst * chunks + c) * msg + start, size)],
            dst_ref=recv_a.at[rows((c * group + me) * msg + start, size)],
            send_sem=send_sem_a, recv_sem=recv_sem_a.at[c], device_id={'w': dst}, device_id_type=MESH)

    def copy_b(off, c, start, size, sem):
        dst = lax.rem(me + off, group)
        return pltpu.make_async_remote_copy(
            src_ref=send_b.at[rows((c * group + dst) * msg + start, size)],
            dst_ref=recv_b.at[rows((c * group + me) * msg + start, size)],
            send_sem=send_sem_b, recv_sem=sem, device_id={'w': dst}, device_id_type=MESH)

    order = [group // 2, 2, group - 2, group // 2 + 1, 3, group - 1, 1]
    order = order if sorted(order) == list(range(1, group)) else list(range(1, group))

    for g in range(GROUPS):
        for copy in loads[g]:
            copy.wait()

        def legendre_body(i, carry):
            m = g * per_group + i
            leg_hi, leg_lo = split(jnp.transpose(leg[m]))
            c_hi, c_lo = split(jnp.concatenate([coef[m, 0], coef[m, 1]], axis=1))
            f = dot(leg_hi, c_hi) + dot(leg_lo, c_hi) + dot(leg_hi, c_lo)
            for t in range(group * lat_loc // SUB):
                re = f[t * SUB:(t + 1) * SUB, :levels]
                im = f[t * SUB:(t + 1) * SUB, levels:]
                send_a[rows((2 * t * wave_loc + m) * SUB, SUB), :] = jnp.where(low, re, pltpu.roll(im, QUAD, 0))
                send_a[rows(((2 * t + 1) * wave_loc + m) * SUB, SUB), :] = jnp.where(low, pltpu.roll(re, QUAD, 0), im)
            return carry

        lax.fori_loop(0, per_group, legendre_body, 0)
        if g == 0:
            pl.semaphore_wait(barrier, group - 1)
        for off in order:
            copy_a(off, 0, g * part, part).start()

    @pl.loop(1, chunks)
    def _(c):
        for off in order:
            copy_a(off, c, 0, msg).start()

    @pl.loop(0, chunks)
    def _(c):
        recv_a[rows((c * group + me) * msg, msg), :] = send_a[rows((me * chunks + c) * msg, msg), :]

    for copy in mats:
        copy.wait()

    @pl.loop(0, chunks)
    def _(c):
        landed = recv_a.at[pl.ds(0, (group - 1) * msg)]
        pltpu.make_async_copy(landed, landed, recv_sem_a.at[c]).wait()

        @pl.loop(0, QUAD // 2)
        def _(pair):
            halves = []
            for u in range(2):
                row = c * (group * msg) + 2 * pair + u
                re = recv_a[pl.ds(row, waves, stride=SUB), :]
                im = recv_a[pl.ds(row + QUAD, waves, stride=SUB), :]
                halves.append(jnp.concatenate([re, im], axis=0))
            f_hi, f_lo = split(jnp.concatenate(halves, axis=1))
            g_val = dot(inv[...], jnp.concatenate([f_hi, f_lo, f_hi], axis=0))
            for u in range(2):
                grid[c * QUAD + 2 * pair + u] = g_val[:, u * levels:(u + 1) * levels]
            q_hi, q_lo = split(g_val * g_val)
            h = dot(fwd[...], jnp.concatenate([q_hi, q_lo, q_hi], axis=0))
            for u in range(2):
                row = c * (group * msg) + 2 * pair + u
                hw = h[:, u * levels:(u + 1) * levels] * wt_ref[me * lat_loc + c * QUAD + 2 * pair + u]
                send_b[pl.ds(row, waves, stride=SUB), :] = hw[:waves]
                send_b[pl.ds(row + QUAD, waves, stride=SUB), :] = hw[waves:]

        @pl.when(c < chunks - 1)
        def _():
            for off in order:
                copy_b(off, c, 0, msg, recv_sem_b).start()

        @pl.when(c == chunks - 1)
        def _():
            for g in range(GROUPS):
                for off in order:
                    copy_b(off, c, g * part, part, last_sem.at[g]).start()

        recv_b[rows((c * group + me) * msg, msg), :] = send_b[rows((c * group + me) * msg, msg), :]

    landed = recv_b.at[pl.ds(0, (chunks - 1) * (group - 1) * msg)]
    pltpu.make_async_copy(landed, landed, recv_sem_b).wait()
    for g in range(GROUPS):
        landed = recv_b.at[pl.ds(0, (group - 1) * part)]
        pltpu.make_async_copy(landed, landed, last_sem.at[g]).wait()

        def back_body(i, carry):
            m = g * per_group + i
            re, im = [], []
            for t in range(group * lat_loc // SUB):
                tiles = []
                for q in (2 * t, 2 * t + 1):
                    s, c = divmod(q, chunks)
                    tiles.append(recv_b[rows(((c * group + s) * wave_loc + m) * SUB, SUB), :])
                a, b = tiles
                re.append(jnp.where(low, a, pltpu.roll(b, QUAD, 0)))
                im.append(jnp.where(low, pltpu.roll(a, QUAD, 0), b))
            h_hi, h_lo = split(jnp.concatenate([jnp.concatenate(re, axis=0), jnp.concatenate(im, axis=0)], axis=1))
            leg_hi, leg_lo = split(leg[m])
            s_val = dot(leg_hi, h_hi) + dot(leg_lo, h_hi) + dot(leg_hi, h_lo)
            spec[m, 0] = s_val[:, :levels]
            spec[m, 1] = s_val[:, levels:]
            return carry

        lax.fori_loop(0, per_group, back_body, 0)

    sent = send_a.at[pl.ds(0, (group - 1) * chunks * msg)]
    pltpu.make_async_copy(sent, sent, send_sem_a).wait()
    pltpu.make_async_copy(sent, sent, send_sem_b).wait()


def solution(mesh):
    group = mesh.shape['w']

    def per_device(coef, legendre, gauss_weight):
        wave_loc, _, levels, degs = coef.shape
        waves = wave_loc * group
        lon = 2 * waves
        lat_loc = legendre.shape[2] // group
        coef_t = jnp.transpose(coef, (0, 1, 3, 2))
        inv, fwd = (jnp.asarray(x) for x in fourier_matrices(waves))
        total = group * lat_loc // QUAD * wave_loc * SUB
        dims = (group, wave_loc, levels, degs, lat_loc, waves, lon)
        hbm = pl.BlockSpec(memory_space=pl.ANY)
        vmem = pl.BlockSpec(memory_space=pltpu.VMEM)
        dma = pltpu.SemaphoreType.DMA
        grid, spec = pl.pallas_call(
            functools.partial(kernel, dims),
            out_shape=(pltpu.VMEM((lat_loc, lon, levels), F32), pltpu.VMEM(coef_t.shape, F32)),
            in_specs=[hbm, hbm, hbm, hbm, pl.BlockSpec(memory_space=pltpu.SMEM)],
            out_specs=(vmem, vmem),
            scratch_shapes=[
                pltpu.VMEM(coef_t.shape, F32),
                pltpu.VMEM((wave_loc, degs, legendre.shape[2]), F32),
                pltpu.VMEM(inv.shape, BF16),
                pltpu.VMEM(fwd.shape, BF16),
                pltpu.VMEM((total, levels), F32),
                pltpu.VMEM((total, levels), F32),
                pltpu.VMEM((total, levels), F32),
                pltpu.VMEM((total, levels), F32),
                dma((2, GROUPS)), dma((2,)), dma, dma((lat_loc // QUAD,)), dma, dma, dma((GROUPS,)),
            ],
            compiler_params=pltpu.CompilerParams(collective_id=0, has_side_effects=True, vmem_limit_bytes=48 * 2**20),
            name='transform_pair',
        )(coef_t, legendre, inv, fwd, gauss_weight)
        return jnp.transpose(grid, (2, 0, 1)), jnp.transpose(spec, (0, 1, 3, 2))

    return jax.shard_map(per_device, mesh=mesh, in_specs=(P('w', None, 'lev', None), P(None, None, None), P(None)), out_specs=(P('lev', 'w', None), P('w', None, 'lev', None)), check_vma=False)
```

```python
import functools

import jax
import jax.numpy as jnp
import ml_dtypes
import numpy as np
from jax import lax
from jax.experimental import pallas as pl
from jax.experimental.pallas import tpu as pltpu
from jax.sharding import PartitionSpec as P

MESH = pl.DeviceIdType.MESH
F32, BF16 = jnp.float32, jnp.bfloat16
SUB = 8
QUAD = 4
SIZES_A = (2, 4, 6, 8)
SIZES_B = (8, 6, 4, 2)
CORES = 2
BLOCK = 4
OWN = 32
RELAYED = 2


def split_np(mat):
    hi = mat.astype(np.float32).astype(ml_dtypes.bfloat16)
    lo = (mat - hi.astype(np.float64)).astype(np.float32).astype(ml_dtypes.bfloat16)
    return hi, lo


def fourier_matrices(waves):
    lon = 2 * waves
    m = np.arange(waves)[:, None]
    n = np.arange(lon)[None, :]
    ang = 2.0 * np.pi * ((m * n) % lon) / lon
    fwd = np.concatenate([np.cos(ang), -np.sin(ang)], axis=0)
    scale = np.where(np.arange(waves) == 0, 1.0, 2.0) / lon
    inv = (fwd * np.tile(scale, 2)[:, None]).T
    out = []
    for mat in (inv, fwd):
        hi, lo = split_np(mat)
        out.append(np.concatenate([hi, hi, lo], axis=1))
    return out


def split(x):
    hi = x.astype(BF16)
    lo = (x - hi.astype(F32)).astype(BF16)
    return hi, lo


def dot(a, b, dims=((1,), (0,))):
    return lax.dot_general(a, b, (dims, ((), ())), preferred_element_type=F32)


def kernel(dims, coef_hbm, leg_hbm, inv_hbm, fwd_hbm, wt_ref, grid, spec,
           coef, leg, inv, fwd, send_a, recv_a, send_b, recv_b,
           tri, leg_tri, spread, leg_own, leg_own_t, part_own, part_mate, part_in, relay,
           load_sem, mat_sem, send_sem_a, recv_sem_a, send_sem_b, recv_sem_b, last_sem,
           tri_load, tri_send, tri_recv, mate_send, mate_recv, part_send, part_recv, relay_send, relay_recv):
    group, wave_loc, levels, degs, lat_loc, waves, lon = dims
    chunks = lat_loc // QUAD
    msg = wave_loc * SUB
    chips = group // CORES
    tri_num = CORES * wave_loc
    tri_m = waves - tri_num
    tri_deg = degs - tri_m
    full = group - CORES
    blocks = wave_loc // BLOCK
    me = lax.axis_index('w')
    core = lax.rem(me, CORES)
    chip = lax.div(me, CORES)
    mate = me + 1 - 2 * core
    is_full = me < full
    is_tri = me >= full

    def starts(sizes):
        return [(g, sum(sizes[:g]), size) for g, size in enumerate(sizes)]

    def rows(start, size):
        return pl.ds(pl.multiple_of(start, SUB), size)

    def skip(b):
        return BLOCK * b // SUB * SUB

    for m in range(tri_num):
        gap = skip(m // BLOCK)
        if gap:
            for r in range(2):
                tri[m, r, 0:gap, :] = jnp.zeros((gap, levels), F32)

    barrier = pltpu.get_barrier_semaphore()
    for off in range(1, group):
        pl.semaphore_signal(barrier, inc=1, device_id={'w': lax.rem(me + off, group)}, device_id_type=MESH)

    def load_pair(g, start, size):
        own = pl.ds(start, size)
        return (pltpu.make_async_copy(coef_hbm.at[own], coef.at[own], load_sem.at[0, g]),
                pltpu.make_async_copy(leg_hbm.at[pl.ds(me * wave_loc + start, size)], leg.at[own], load_sem.at[1, g]))

    def load_block(b):
        gap = skip(b)
        return pltpu.make_async_copy(
            coef_hbm.at[pl.ds(BLOCK * (b % blocks), BLOCK), :, pl.ds(tri_m + gap, tri_deg - gap), :],
            tri.at[pl.ds(BLOCK * b, BLOCK), :, pl.ds(gap, tri_deg - gap), :], tri_load.at[b])

    @pl.when(is_full)
    def _():
        for args in starts(SIZES_A):
            for copy in load_pair(*args):
                copy.start()

    for b in range(CORES * blocks):
        @pl.when(me == full + b // blocks)
        def _():
            load_block(b).start()

    leg_tri_copy = pltpu.make_async_copy(leg_hbm.at[pl.ds(tri_m, tri_num), pl.ds(tri_m, tri_deg), :], leg_tri, mat_sem.at[2])
    mats = [leg_tri_copy, pltpu.make_async_copy(inv_hbm, inv, mat_sem.at[0]), pltpu.make_async_copy(fwd_hbm, fwd, mat_sem.at[1])]
    for copy in mats:
        copy.start()

    low = lax.broadcasted_iota(jnp.int32, (SUB, levels), 0) < QUAD

    def copy_a(off, c, start, size):
        dst = lax.rem(me + off, group)
        return pltpu.make_async_remote_copy(
            src_ref=send_a.at[rows((dst * chunks + c) * msg + start, size)],
            dst_ref=recv_a.at[rows((c * group + me) * msg + start, size)],
            send_sem=send_sem_a, recv_sem=recv_sem_a.at[c], device_id={'w': dst}, device_id_type=MESH)

    def copy_b(dst, c, start, size, sem):
        return pltpu.make_async_remote_copy(
            src_ref=send_b.at[rows((c * group + dst) * msg + start, size)],
            dst_ref=recv_b.at[rows((c * group + me) * msg + start, size)],
            send_sem=send_sem_b, recv_sem=sem, device_id={'w': dst}, device_id_type=MESH)

    def copy_relay(dst, c):
        slot = c * CORES + lax.rem(dst, CORES)
        return pltpu.make_async_remote_copy(
            src_ref=send_b.at[rows((c * group + dst) * msg, msg)], dst_ref=relay.at[rows(slot * msg, msg)],
            send_sem=send_sem_b, recv_sem=relay_recv.at[slot], device_id={'w': full + core}, device_id_type=MESH)

    def copy_onward(c, e):
        slot = c * CORES + e
        return pltpu.make_async_remote_copy(
            src_ref=relay.at[rows(slot * msg, msg)], dst_ref=recv_b.at[rows((c * group + core) * msg, msg)],
            send_sem=relay_send, recv_sem=recv_sem_b, device_id={'w': group // 2 + e}, device_id_type=MESH)

    def copy_tri(b, lane, dst):
        gap = skip(b)
        ref = tri.at[pl.ds(BLOCK * b, BLOCK), :, pl.ds(gap, tri_deg - gap), :]
        return pltpu.make_async_remote_copy(
            src_ref=ref, dst_ref=ref, send_sem=tri_send.at[lane, b % blocks], recv_sem=tri_recv.at[b],
            device_id={'w': dst}, device_id_type=MESH)

    def copy_mate(b):
        gap = skip(b)
        return pltpu.make_async_remote_copy(
            src_ref=part_own.at[pl.ds(BLOCK * b, BLOCK), :, pl.ds(gap, tri_deg - gap), :],
            dst_ref=part_mate.at[pl.ds(BLOCK * (b % blocks), BLOCK), :, pl.ds(gap, tri_deg - gap), :],
            send_sem=mate_send.at[b], recv_sem=mate_recv.at[b], device_id={'w': mate}, device_id_type=MESH)

    def copy_part(b):
        gap = skip(b)
        return pltpu.make_async_remote_copy(
            src_ref=part_own.at[pl.ds(BLOCK * b, BLOCK), :, pl.ds(gap, tri_deg - gap), :],
            dst_ref=part_in.at[chip, pl.ds(BLOCK * (b % blocks), BLOCK), :, pl.ds(gap, tri_deg - gap), :],
            send_sem=part_send.at[b], recv_sem=part_recv.at[chip, b], device_id={'w': full + core}, device_id_type=MESH)

    def wait_rows(ref, sem, count):
        landed = ref.at[pl.ds(0, count)]
        pltpu.make_async_copy(landed, landed, sem).wait()

    order = [group // 2, 2, group - 2, group // 2 + 1, 3, group - 1, 1]
    order = order if sorted(order) == list(range(1, group)) else list(range(1, group))

    @pl.when(is_full)
    def _():
        for g, start, size in starts(SIZES_A):
            for copy in load_pair(g, start, size):
                copy.wait()

            def legendre_body(i, carry):
                m = start + i
                leg_hi, leg_lo = split(jnp.transpose(leg[m]))
                c_hi, c_lo = split(jnp.concatenate([coef[m, 0], coef[m, 1]], axis=1))
                f = dot(leg_hi, c_hi) + dot(leg_lo, c_hi) + dot(leg_hi, c_lo)
                for t in range(group * lat_loc // SUB):
                    re = f[t * SUB:(t + 1) * SUB, :levels]
                    im = f[t * SUB:(t + 1) * SUB, levels:]
                    send_a[rows((2 * t * wave_loc + m) * SUB, SUB), :] = jnp.where(low, re, pltpu.roll(im, QUAD, 0))
                    send_a[rows(((2 * t + 1) * wave_loc + m) * SUB, SUB), :] = jnp.where(low, pltpu.roll(re, QUAD, 0), im)
                return carry

            lax.fori_loop(0, size, legendre_body, 0)
            if g == 0:
                pl.semaphore_wait(barrier, group - 1)
            for off in order:
                copy_a(off, 0, start * SUB, size * SUB).start()

        @pl.loop(1, chunks)
        def _(c):
            for off in order:
                copy_a(off, c, 0, msg).start()

        @pl.loop(0, chunks)
        def _(c):
            recv_a[rows((c * group + me) * msg, msg), :] = send_a[rows((me * chunks + c) * msg, msg), :]

    @pl.when(is_tri)
    def _():
        pl.semaphore_wait(barrier, group - 1)
        for b in range(CORES * blocks):
            @pl.when(core == b // blocks)
            def _():
                load_block(b).wait()
                for lane, dst in enumerate([CORES + core, core, 2 * CORES + core, mate]):
                    copy_tri(b, lane, dst).start()

    leg_tri_copy.wait()
    lat_all = group * lat_loc

    def spread_body(m, carry):
        x = jnp.concatenate([leg_tri[m], jnp.zeros((levels - tri_deg, lat_all), F32)], axis=0)
        eighth, lane = m // SUB, lax.rem(m, SUB)
        spread[pl.ds(eighth * lat_all * SUB + lane, lat_all, stride=SUB), :] = jnp.transpose(x)
        return carry

    lax.fori_loop(0, tri_num, spread_body, 0)

    def own_body(m, carry):
        eighth, lane = m // SUB, lax.rem(m, SUB)
        own = spread[pl.ds((eighth * lat_all + me * lat_loc) * SUB + lane, OWN, stride=SUB), :]
        own = jnp.where(lax.broadcasted_iota(jnp.int32, (OWN, levels), 0) < lat_loc, own, 0.0)
        leg_own[m] = own
        leg_own_t[m] = jnp.transpose(own)[:tri_deg]
        return carry

    lax.fori_loop(0, tri_num, own_body, 0)

    for b in range(CORES * blocks):
        @pl.when(jnp.logical_and(is_full, core == b // blocks))
        def _():
            copy_tri(b, 3, mate).wait_recv()
            copy_tri(b, 3, mate).start()
    for b in range(CORES * blocks):
        @pl.when(core != b // blocks)
        def _():
            copy_tri(b, 3, mate).wait_recv()

    def tri_body(m, carry):
        own_hi, own_lo = split(leg_own[m][:, :tri_deg])
        c_hi, c_lo = split(jnp.concatenate([tri[m, 0], tri[m, 1]], axis=1))
        f = dot(own_hi, c_hi) + dot(own_lo, c_hi) + dot(own_hi, c_lo)
        for c in range(chunks):
            t = c // 2
            re = f[t * SUB:(t + 1) * SUB, :levels]
            im = f[t * SUB:(t + 1) * SUB, levels:]
            tile = jnp.where(low, pltpu.roll(re, QUAD, 0), im) if c % 2 else jnp.where(low, re, pltpu.roll(im, QUAD, 0))
            recv_a[rows(((c * group + full) * wave_loc + m) * SUB, SUB), :] = tile
        return carry

    lax.fori_loop(0, tri_num, tri_body, 0)

    for copy in mats[1:]:
        copy.wait()

    @pl.loop(0, chunks)
    def _(c):
        @pl.when(is_full)
        def _():
            wait_rows(recv_a, recv_sem_a.at[c], (full - 1) * msg)

        @pl.when(is_tri)
        def _():
            wait_rows(recv_a, recv_sem_a.at[c], full * msg)

        @pl.loop(0, QUAD // 2)
        def _(pair):
            halves = []
            for u in range(2):
                row = c * (group * msg) + 2 * pair + u
                re = recv_a[pl.ds(row, waves, stride=SUB), :]
                im = recv_a[pl.ds(row + QUAD, waves, stride=SUB), :]
                halves.append(jnp.concatenate([re, im], axis=0))
            f_hi, f_lo = split(jnp.concatenate(halves, axis=1))
            g_val = dot(inv[...], jnp.concatenate([f_hi, f_lo, f_hi], axis=0))
            for u in range(2):
                grid[c * QUAD + 2 * pair + u] = g_val[:, u * levels:(u + 1) * levels]
            q_hi, q_lo = split(g_val * g_val)
            h = dot(fwd[...], jnp.concatenate([q_hi, q_lo, q_hi], axis=0))
            for u in range(2):
                row = c * (group * msg) + 2 * pair + u
                hw = h[:, u * levels:(u + 1) * levels] * wt_ref[me * lat_loc + c * QUAD + 2 * pair + u]
                send_b[pl.ds(row, waves, stride=SUB), :] = hw[:waves]
                send_b[pl.ds(row + QUAD, waves, stride=SUB), :] = hw[waves:]

        @pl.when(c < chunks - 1)
        def _():
            for off in order:
                dst = lax.rem(me + off, group)
                by_relay = jnp.logical_and(jnp.logical_and(chip == 0, dst >= group // 2), c < RELAYED)

                @pl.when(jnp.logical_and(dst < full, by_relay))
                def _():
                    copy_relay(dst, c).start()

                @pl.when(jnp.logical_and(dst < full, jnp.logical_not(by_relay)))
                def _():
                    copy_b(dst, c, 0, msg, recv_sem_b).start()

        @pl.when(c == chunks - 1)
        def _():
            for g, start, size in starts(SIZES_B):
                for off in order:
                    dst = lax.rem(me + off, group)

                    @pl.when(dst < full)
                    def _():
                        copy_b(dst, c, start * SUB, size * SUB, last_sem.at[g]).start()

        @pl.when(is_full)
        def _():
            recv_b[rows((c * group + me) * msg, msg), :] = send_b[rows((c * group + me) * msg, msg), :]

    zero = jnp.zeros((SUB, levels), F32)

    def part_body(i, carry):
        m = lax.rem(i + (1 - core) * wave_loc, tri_num)
        re, im = [], []
        for t in range(OWN // SUB):
            a, b = (send_b[rows((c * waves + tri_m + m) * SUB, SUB), :] if c < chunks else zero for c in (2 * t, 2 * t + 1))
            re.append(jnp.where(low, a, pltpu.roll(b, QUAD, 0)))
            im.append(jnp.where(low, pltpu.roll(a, QUAD, 0), b))
        h_hi, h_lo = split(jnp.concatenate([jnp.concatenate(re, axis=0), jnp.concatenate(im, axis=0)], axis=1))
        own_hi, own_lo = split(leg_own_t[m])
        p_val = dot(own_hi, h_hi) + dot(own_lo, h_hi) + dot(own_hi, h_lo)
        part_own[m, 0] = p_val[:, :levels]
        part_own[m, 1] = p_val[:, levels:]
        return carry

    lax.fori_loop(0, wave_loc, part_body, 0)
    for b in range(CORES * blocks):
        @pl.when(core != b // blocks)
        def _():
            copy_mate(b).start()
    lax.fori_loop(wave_loc, tri_num, part_body, 0)
    for b in range(CORES * blocks):
        @pl.when(core == b // blocks)
        def _():
            copy_mate(b).wait_recv()

            @pl.loop(0, BLOCK)
            def _(i):
                gap = skip(b)
                for r in range(2):
                    part_own[BLOCK * b + i, r, gap:, :] += part_mate[BLOCK * (b % blocks) + i, r, gap:, :]

        @pl.when(jnp.logical_and(is_full, core == b // blocks))
        def _():
            copy_part(b).start()

    @pl.when(is_tri)
    def _():
        for c in range(RELAYED):
            for e in range(CORES):
                slot = c * CORES + e
                landed = relay.at[pl.ds(slot * msg, msg)]
                pltpu.make_async_copy(landed, landed, relay_recv.at[slot]).wait()
                copy_onward(c, e).start()

    @pl.when(is_full)
    def _():
        wait_rows(recv_b, recv_sem_b, (chunks - 1) * (group - 1) * msg)
        for g, start, size in starts(SIZES_B):
            wait_rows(recv_b, last_sem.at[g], (group - 1) * size * SUB)

            def back_body(i, carry):
                m = start + i
                re, im = [], []
                for t in range(group * lat_loc // SUB):
                    tiles = []
                    for q in (2 * t, 2 * t + 1):
                        s, c = divmod(q, chunks)
                        tiles.append(recv_b[rows(((c * group + s) * wave_loc + m) * SUB, SUB), :])
                    a, b = tiles
                    re.append(jnp.where(low, a, pltpu.roll(b, QUAD, 0)))
                    im.append(jnp.where(low, pltpu.roll(a, QUAD, 0), b))
                h_hi, h_lo = split(jnp.concatenate([jnp.concatenate(re, axis=0), jnp.concatenate(im, axis=0)], axis=1))
                leg_hi, leg_lo = split(leg[m])
                s_val = dot(leg_hi, h_hi) + dot(leg_lo, h_hi) + dot(leg_hi, h_lo)
                spec[m, 0] = s_val[:, :levels]
                spec[m, 1] = s_val[:, levels:]
                return carry

            lax.fori_loop(0, size, back_body, 0)

    for b in range(CORES * blocks):
        @pl.when(me == full + b // blocks)
        def _():
            gap = skip(b)
            for src in range(chips - 1):
                landed = part_in.at[src, pl.ds(BLOCK * (b % blocks), BLOCK), :, pl.ds(gap, tri_deg - gap), :]
                pltpu.make_async_copy(landed, landed, part_recv.at[src, b]).wait()

            @pl.loop(0, BLOCK)
            def _(i):
                m = BLOCK * (b % blocks) + i
                for r in range(2):
                    acc = part_own[BLOCK * b + i, r, gap:, :]
                    for src in range(chips - 1):
                        acc = acc + part_in[src, m, r, gap:, :]
                    spec[m, r, :tri_m + gap, :] = jnp.zeros((tri_m + gap, levels), F32)
                    spec[m, r, tri_m + gap:, :] = acc

    @pl.when(is_full)
    def _():
        wait_rows(send_a, send_sem_a, (group - 1) * chunks * msg)
        wait_rows(send_b, send_sem_b, (full - 1) * chunks * msg)

    @pl.when(is_tri)
    def _():
        wait_rows(send_b, send_sem_b, full * chunks * msg)
        wait_rows(relay, relay_send, RELAYED * CORES * msg)

    for b in range(CORES * blocks):
        @pl.when(core == b // blocks)
        def _():
            copy_tri(b, 3, mate).wait_send()

        @pl.when(core != b // blocks)
        def _():
            copy_mate(b).wait_send()

        @pl.when(me == full + b // blocks)
        def _():
            for lane in range(3):
                copy_tri(b, lane, mate).wait_send()

        @pl.when(jnp.logical_and(is_full, core == b // blocks))
        def _():
            copy_part(b).wait_send()


def solution(mesh):
    group = mesh.shape['w']

    def per_device(coef, legendre, gauss_weight):
        wave_loc, _, levels, degs = coef.shape
        waves = wave_loc * group
        lon = 2 * waves
        lat_loc = legendre.shape[2] // group
        coef_t = jnp.transpose(coef, (0, 1, 3, 2))
        inv, fwd = (jnp.asarray(x) for x in fourier_matrices(waves))
        tri_num = CORES * wave_loc
        tri_deg = degs - waves + tri_num
        blocks = tri_num // BLOCK
        total = group * lat_loc // QUAD * wave_loc * SUB
        dims = (group, wave_loc, levels, degs, lat_loc, waves, lon)
        hbm = pl.BlockSpec(memory_space=pl.ANY)
        vmem = pl.BlockSpec(memory_space=pltpu.VMEM)
        dma = pltpu.SemaphoreType.DMA
        grid, spec = pl.pallas_call(
            functools.partial(kernel, dims),
            out_shape=(pltpu.VMEM((lat_loc, lon, levels), F32), pltpu.VMEM(coef_t.shape, F32)),
            in_specs=[hbm, hbm, hbm, hbm, pl.BlockSpec(memory_space=pltpu.SMEM)],
            out_specs=(vmem, vmem),
            scratch_shapes=[
                pltpu.VMEM(coef_t.shape, F32),
                pltpu.VMEM((wave_loc, degs, legendre.shape[2]), F32),
                pltpu.VMEM(inv.shape, BF16),
                pltpu.VMEM(fwd.shape, BF16),
                pltpu.VMEM((total, levels), F32),
                pltpu.VMEM((total, levels), F32),
                pltpu.VMEM((total, levels), F32),
                pltpu.VMEM((total, levels), F32),
                pltpu.VMEM((tri_num, 2, tri_deg, levels), F32),
                pltpu.VMEM((tri_num, tri_deg, legendre.shape[2]), F32),
                pltpu.VMEM((tri_num * legendre.shape[2] + OWN * SUB, levels), F32),
                pltpu.VMEM((tri_num, OWN, levels), F32),
                pltpu.VMEM((tri_num, tri_deg, OWN), F32),
                pltpu.VMEM((tri_num, 2, tri_deg, levels), F32),
                pltpu.VMEM((wave_loc, 2, tri_deg, levels), F32),
                pltpu.VMEM((group // CORES - 1, wave_loc, 2, tri_deg, levels), F32),
                pltpu.VMEM((RELAYED * CORES * wave_loc * SUB, levels), F32),
                dma((2, len(SIZES_A))), dma((3,)), dma, dma((lat_loc // QUAD,)), dma, dma, dma((len(SIZES_B),)),
                dma((blocks,)), dma((4, blocks // CORES)), dma((blocks,)), dma((blocks,)), dma((blocks,)),
                dma((blocks,)), dma((group // CORES - 1, blocks)), dma, dma((RELAYED * CORES,)),
            ],
            compiler_params=pltpu.CompilerParams(collective_id=0, has_side_effects=True, vmem_limit_bytes=48 * 2**20),
            name='transform_pair',
        )(coef_t, legendre, inv, fwd, gauss_weight)
        return jnp.transpose(grid, (2, 0, 1)), jnp.transpose(spec, (0, 1, 3, 2))

    return jax.shard_map(per_device, mesh=mesh, in_specs=(P('w', None, 'lev', None), P(None, None, None), P(None)), out_specs=(P('lev', 'w', None), P('w', None, 'lev', None)), check_vma=False)
```

```python
import functools

import jax
import jax.numpy as jnp
import ml_dtypes
import numpy as np
from jax import lax
from jax.experimental import pallas as pl
from jax.experimental.pallas import tpu as pltpu
from jax.sharding import PartitionSpec as P

MESH = pl.DeviceIdType.MESH
F32, BF16 = jnp.float32, jnp.bfloat16
SUB = 8
QUAD = 4
SIZES_A = (4, 4, 4, 8)
EARLY = 2
SIZES_B = (8, 6, 4, 2)
CORES = 2
BLOCK = 4
OWN = 32
HELD = 2
LAG = 2
RELAYED = 2


def split_np(mat):
    hi = mat.astype(np.float32).astype(ml_dtypes.bfloat16)
    lo = (mat - hi.astype(np.float64)).astype(np.float32).astype(ml_dtypes.bfloat16)
    return hi, lo


def fourier_matrices(waves):
    lon = 2 * waves
    m = np.arange(waves)[:, None]
    n = np.arange(lon)[None, :]
    ang = 2.0 * np.pi * ((m * n) % lon) / lon
    fwd = np.concatenate([np.cos(ang), -np.sin(ang)], axis=0)
    scale = np.where(np.arange(waves) == 0, 1.0, 2.0) / lon
    inv = (fwd * np.tile(scale, 2)[:, None]).T
    out = []
    for mat in (inv, fwd):
        hi, lo = split_np(mat)
        out.append(np.concatenate([hi, hi, lo], axis=1))
    return out


def split(x):
    hi = x.astype(BF16)
    lo = (x - hi.astype(F32)).astype(BF16)
    return hi, lo


def dot(a, b, dims=((1,), (0,))):
    return lax.dot_general(a, b, (dims, ((), ())), preferred_element_type=F32)


def kernel(dims, coef_hbm, leg_hbm, inv_hbm, fwd_hbm, wt_ref, grid, spec,
           coef, leg, inv, fwd, send_a, recv_a, send_b, recv_b,
           tri, leg_tri, leg_own, leg_own_t, part_own, part_mate, part_in, relay,
           load_sem, mat_sem, send_sem_a, recv_sem_a, send_sem_b, recv_sem_b, last_sem,
           tri_load, tri_send, tri_recv, mate_send, mate_recv, part_send, part_recv, relay_send, relay_recv):
    group, wave_loc, levels, degs, lat_loc, waves, lon = dims
    chunks = lat_loc // QUAD
    msg = wave_loc * SUB
    chips = group // CORES
    tri_num = CORES * wave_loc
    tri_m = waves - tri_num
    tri_deg = degs - tri_m
    full = group - CORES
    blocks = wave_loc // BLOCK
    me = lax.axis_index('w')
    core = lax.rem(me, CORES)
    chip = lax.div(me, CORES)
    mate = me + 1 - 2 * core
    is_full = me < full
    is_tri = me >= full
    forwards = chip == chips - 2

    def starts(sizes):
        return [(g, sum(sizes[:g]), size) for g, size in enumerate(sizes)]

    def rows(start, size):
        return pl.ds(pl.multiple_of(start, SUB), size)

    def skip(b):
        return BLOCK * b // SUB * SUB

    for m in range(tri_num):
        gap = skip(m // BLOCK)
        if gap:
            for r in range(2):
                tri[m, r, 0:gap, :] = jnp.zeros((gap, levels), F32)

    barrier = pltpu.get_barrier_semaphore()
    for off in range(1, group):
        pl.semaphore_signal(barrier, inc=1, device_id={'w': lax.rem(me + off, group)}, device_id_type=MESH)

    def load_pair(g, start, size):
        own = pl.ds(start, size)
        return (pltpu.make_async_copy(coef_hbm.at[own], coef.at[own], load_sem.at[0, g]),
                pltpu.make_async_copy(leg_hbm.at[pl.ds(me * wave_loc + start, size)], leg.at[own], load_sem.at[1, g]))

    def load_block(b):
        gap = skip(b)
        return pltpu.make_async_copy(
            coef_hbm.at[pl.ds(BLOCK * (b % blocks), BLOCK), :, pl.ds(tri_m + gap, tri_deg - gap), :],
            tri.at[pl.ds(BLOCK * b, BLOCK), :, pl.ds(gap, tri_deg - gap), :], tri_load.at[b])

    @pl.when(is_full)
    def _():
        for args in starts(SIZES_A):
            for copy in load_pair(*args):
                copy.start()

    for b in range(CORES * blocks):
        @pl.when(me == full + b // blocks)
        def _():
            load_block(b).start()

    leg_tri_copy = pltpu.make_async_copy(leg_hbm.at[pl.ds(tri_m, tri_num), pl.ds(tri_m, tri_deg), :], leg_tri, mat_sem.at[2])
    mats = [leg_tri_copy, pltpu.make_async_copy(inv_hbm, inv, mat_sem.at[0]), pltpu.make_async_copy(fwd_hbm, fwd, mat_sem.at[1])]
    for copy in mats:
        copy.start()

    low = lax.broadcasted_iota(jnp.int32, (SUB, levels), 0) < QUAD

    def copy_a(off, c, start, size):
        dst = lax.rem(me + off, group)
        return pltpu.make_async_remote_copy(
            src_ref=send_a.at[rows((dst * chunks + c) * msg + start, size)],
            dst_ref=recv_a.at[rows((c * group + me) * msg + start, size)],
            send_sem=send_sem_a, recv_sem=recv_sem_a.at[c], device_id={'w': dst}, device_id_type=MESH)

    def copy_b(dst, c, start, size, sem):
        return pltpu.make_async_remote_copy(
            src_ref=send_b.at[rows((c * group + dst) * msg + start, size)],
            dst_ref=recv_b.at[rows((c * group + me) * msg + start, size)],
            send_sem=send_sem_b, recv_sem=sem, device_id={'w': dst}, device_id_type=MESH)

    def after_parts(dst, c):
        return jnp.logical_and(jnp.logical_and(chip == 1, dst < CORES), c >= HELD)

    def copy_relay(dst, c):
        slot = c * CORES + lax.rem(dst, CORES)
        return pltpu.make_async_remote_copy(
            src_ref=send_b.at[rows((c * group + dst) * msg, msg)], dst_ref=relay.at[rows(slot * msg, msg)],
            send_sem=send_sem_b, recv_sem=relay_recv.at[slot], device_id={'w': full + core}, device_id_type=MESH)

    def copy_onward(c, e):
        slot = c * CORES + e
        return pltpu.make_async_remote_copy(
            src_ref=relay.at[rows(slot * msg, msg)], dst_ref=recv_b.at[rows((c * group + core) * msg, msg)],
            send_sem=relay_send, recv_sem=recv_sem_b.at[c], device_id={'w': group // 2 + e}, device_id_type=MESH)

    def copy_tri(b, lane, dst):
        gap = skip(b)
        ref = tri.at[pl.ds(BLOCK * b, BLOCK), :, pl.ds(gap, tri_deg - gap), :]
        return pltpu.make_async_remote_copy(
            src_ref=ref, dst_ref=ref, send_sem=tri_send.at[lane, b], recv_sem=tri_recv.at[b],
            device_id={'w': dst}, device_id_type=MESH)

    def entry(b, at):
        return (b // CORES if at == 1 else b) % CORES

    def gets(b):
        return jnp.where(chip == 1, entry(b, 1), entry(b, 0)) == core

    def keeps(b):
        return jnp.where(is_tri, b // blocks, b % CORES) == core

    def mate_slot(b):
        return jnp.where(is_tri, b % blocks, b // CORES)

    def copy_mate(b):
        gap = skip(b)
        return pltpu.make_async_remote_copy(
            src_ref=part_own.at[pl.ds(BLOCK * b, BLOCK), :, pl.ds(gap, tri_deg - gap), :],
            dst_ref=part_mate.at[pl.ds(BLOCK * mate_slot(b), BLOCK), :, pl.ds(gap, tri_deg - gap), :],
            send_sem=mate_send.at[b], recv_sem=mate_recv.at[b], device_id={'w': mate}, device_id_type=MESH)

    def copy_part(b):
        gap = skip(b)
        to_first = chip == 1
        slot = jnp.where(chip == chips - 2, 1, 0)
        dst = jnp.where(to_first, core, full + b // blocks)
        return pltpu.make_async_remote_copy(
            src_ref=part_own.at[pl.ds(BLOCK * b, BLOCK), :, pl.ds(gap, tri_deg - gap), :],
            dst_ref=part_in.at[slot, pl.ds(BLOCK * (b % blocks), BLOCK), :, pl.ds(gap, tri_deg - gap), :],
            send_sem=part_send.at[b], recv_sem=part_recv.at[slot, b], device_id={'w': dst}, device_id_type=MESH)

    def wait_part(b, slot):
        gap = skip(b)
        landed = part_in.at[slot, pl.ds(BLOCK * (b % blocks), BLOCK), :, pl.ds(gap, tri_deg - gap), :]
        pltpu.make_async_copy(landed, landed, part_recv.at[slot, b]).wait()

    def wait_rows(ref, sem, count):
        landed = ref.at[pl.ds(0, count)]
        pltpu.make_async_copy(landed, landed, sem).wait()

    order = [group // 2, 2, group - 2, group // 2 + 1, 3, group - 1, 1]
    order = order if sorted(order) == list(range(1, group)) else list(range(1, group))

    def held(off, c):
        dst_chip = lax.div(lax.rem(me + off, group), CORES)
        return jnp.logical_and(forwards, jnp.logical_or(dst_chip == 0, jnp.logical_and(dst_chip == 1, c >= HELD)))

    @pl.when(is_full)
    def _():
        for g, start, size in starts(SIZES_A):
            for copy in load_pair(g, start, size):
                copy.wait()

            def legendre_body(i, carry):
                m = start + i
                leg_hi, leg_lo = split(jnp.transpose(leg[m]))
                c_hi, c_lo = split(jnp.concatenate([coef[m, 0], coef[m, 1]], axis=1))
                f = dot(leg_hi, c_hi) + dot(leg_lo, c_hi) + dot(leg_hi, c_lo)
                for t in range(group * lat_loc // SUB):
                    re = f[t * SUB:(t + 1) * SUB, :levels]
                    im = f[t * SUB:(t + 1) * SUB, levels:]
                    send_a[rows((2 * t * wave_loc + m) * SUB, SUB), :] = jnp.where(low, re, pltpu.roll(im, QUAD, 0))
                    send_a[rows(((2 * t + 1) * wave_loc + m) * SUB, SUB), :] = jnp.where(low, pltpu.roll(re, QUAD, 0), im)
                return carry

            lax.fori_loop(0, size, legendre_body, 0, unroll=4)
            if g == 0:
                pl.semaphore_wait(barrier, group - 1)
            for off in order:
                copy_a(off, 0, start * SUB, size * SUB).start()
            if g < EARLY:
                for off in order:
                    @pl.when(jnp.logical_not(held(off, 1)))
                    def _():
                        copy_a(off, 1, start * SUB, size * SUB).start()

        rest = sum(SIZES_A[:EARLY])
        for off in order:
            @pl.when(jnp.logical_not(held(off, 1)))
            def _():
                copy_a(off, 1, rest * SUB, (wave_loc - rest) * SUB).start()

        @pl.loop(2, chunks)
        def _(c):
            for off in order:
                @pl.when(jnp.logical_not(held(off, c)))
                def _():
                    copy_a(off, c, 0, msg).start()

        @pl.loop(0, chunks)
        def _(c):
            recv_a[rows((c * group + me) * msg, msg), :] = send_a[rows((me * chunks + c) * msg, msg), :]

    @pl.when(is_tri)
    def _():
        pl.semaphore_wait(barrier, group - 1)
        for b in range(CORES * blocks):
            @pl.when(core == b // blocks)
            def _():
                load_block(b).wait()
                for lane, dst in enumerate([full - CORES + entry(b, chips - 2), entry(b, 0), mate]):
                    copy_tri(b, lane, dst).start()

    @pl.when(forwards)
    def _():
        for b in range(CORES * blocks):
            @pl.when(gets(b))
            def _():
                copy_tri(b, 2, mate).wait_recv()
                copy_tri(b, 0, full - 2 * CORES + entry(b, 1)).start()
                copy_tri(b, 2, mate).start()

        @pl.loop(1, chunks)
        def _(c):
            for off in order:
                @pl.when(held(off, c))
                def _():
                    copy_a(off, c, 0, msg).start()

    leg_tri_copy.wait()
    lat_all = group * lat_loc

    pick = lax.broadcasted_iota(jnp.int32, (lat_all, OWN), 0) == lax.broadcasted_iota(jnp.int32, (lat_all, OWN), 1) + me * lat_loc
    pick = jnp.logical_and(pick, lax.broadcasted_iota(jnp.int32, (lat_all, OWN), 1) < lat_loc)
    pick = jnp.where(pick, 1.0, 0.0).astype(BF16)

    def own_body(m, carry):
        for half, value in enumerate(split(leg_tri[m])):
            mine = dot(value, pick)
            leg_own_t[half, m] = mine.astype(BF16)
            leg_own[half, m] = jnp.transpose(mine).astype(BF16)
        return carry

    lax.fori_loop(0, tri_num, own_body, 0, unroll=4)

    for b in range(CORES * blocks):
        @pl.when(jnp.logical_and(jnp.logical_and(is_full, jnp.logical_not(forwards)), gets(b)))
        def _():
            copy_tri(b, 2, mate).wait_recv()
            copy_tri(b, 2, mate).start()

    for b in range(CORES * blocks):
        @pl.when(jnp.logical_not(jnp.where(is_tri, core == b // blocks, gets(b))))
        def _():
            copy_tri(b, 2, mate).wait_recv()

    def tri_body(m, carry):
        own_hi, own_lo = leg_own[0, m], leg_own[1, m]
        c_hi, c_lo = split(jnp.concatenate([tri[m, 0], tri[m, 1]], axis=1))
        f = dot(own_hi, c_hi) + dot(own_lo, c_hi) + dot(own_hi, c_lo)
        for c in range(chunks):
            t = c // 2
            re = f[t * SUB:(t + 1) * SUB, :levels]
            im = f[t * SUB:(t + 1) * SUB, levels:]
            tile = jnp.where(low, pltpu.roll(re, QUAD, 0), im) if c % 2 else jnp.where(low, re, pltpu.roll(im, QUAD, 0))
            recv_a[rows(((c * group + full) * wave_loc + m) * SUB, SUB), :] = tile
        return carry

    lax.fori_loop(0, tri_num, tri_body, 0, unroll=4)

    for copy in mats[1:]:
        copy.wait()

    @pl.loop(0, chunks)
    def _(c):
        @pl.when(is_full)
        def _():
            wait_rows(recv_a, recv_sem_a.at[c], (full - 1) * msg)

        @pl.when(is_tri)
        def _():
            wait_rows(recv_a, recv_sem_a.at[c], full * msg)

        @pl.loop(0, QUAD // 2)
        def _(pair):
            halves = []
            for u in range(2):
                row = c * (group * msg) + 2 * pair + u
                re = recv_a[pl.ds(row, waves, stride=SUB), :]
                im = recv_a[pl.ds(row + QUAD, waves, stride=SUB), :]
                halves.append(jnp.concatenate([re, im], axis=0))
            f_hi, f_lo = split(jnp.concatenate(halves, axis=1))
            g_val = dot(inv[...], jnp.concatenate([f_hi, f_lo, f_hi], axis=0))
            for u in range(2):
                grid[c * QUAD + 2 * pair + u] = g_val[:, u * levels:(u + 1) * levels]
            q_hi, q_lo = split(g_val * g_val)
            h = dot(fwd[...], jnp.concatenate([q_hi, q_lo, q_hi], axis=0))
            for u in range(2):
                row = c * (group * msg) + 2 * pair + u
                hw = h[:, u * levels:(u + 1) * levels] * wt_ref[me * lat_loc + c * QUAD + 2 * pair + u]
                send_b[pl.ds(row, waves, stride=SUB), :] = hw[:waves]
                send_b[pl.ds(row + QUAD, waves, stride=SUB), :] = hw[waves:]

        @pl.when(c < chunks - 1)
        def _():
            for off in order:
                dst = lax.rem(me + off, group)
                by_relay = jnp.logical_and(jnp.logical_and(chip == 0, dst >= group // 2), c < RELAYED)

                @pl.when(jnp.logical_and(dst < full, by_relay))
                def _():
                    copy_relay(dst, c).start()

                late = jnp.logical_and(is_tri, lax.div(dst, CORES) == 1)

                ready = jnp.logical_and(jnp.logical_or(jnp.logical_not(late), c >= LAG), jnp.logical_not(after_parts(dst, c)))

                @pl.when(jnp.logical_and(jnp.logical_and(dst < full, jnp.logical_not(by_relay)), ready))
                def _():
                    copy_b(dst, c, 0, msg, recv_sem_b.at[c]).start()

                @pl.when(jnp.logical_and(late, c == LAG))
                def _():
                    for before in range(LAG):
                        copy_b(dst, before, 0, msg, recv_sem_b.at[before]).start()

        @pl.when(is_full)
        def _():
            recv_b[rows((c * group + me) * msg, msg), :] = send_b[rows((c * group + me) * msg, msg), :]

    zero = jnp.zeros((SUB, levels), F32)

    def part_body(i, carry):
        side = jnp.where(i < wave_loc, 1 - core, core)
        spread = BLOCK * (CORES * lax.div(lax.rem(i, wave_loc), BLOCK) + side) + lax.rem(i, BLOCK)
        m = jnp.where(is_tri, lax.rem(i, wave_loc) + side * wave_loc, spread)
        re, im = [], []
        for t in range(OWN // SUB):
            a, b = (send_b[rows((c * waves + tri_m + m) * SUB, SUB), :] if c < chunks else zero for c in (2 * t, 2 * t + 1))
            re.append(jnp.where(low, a, pltpu.roll(b, QUAD, 0)))
            im.append(jnp.where(low, pltpu.roll(a, QUAD, 0), b))
        h_hi, h_lo = split(jnp.concatenate([jnp.concatenate(re, axis=0), jnp.concatenate(im, axis=0)], axis=1))
        own_hi, own_lo = leg_own_t[0, m], leg_own_t[1, m]
        p_val = dot(own_hi, h_hi) + dot(own_lo, h_hi) + dot(own_hi, h_lo)
        part_own[m, 0] = p_val[:, :levels]
        part_own[m, 1] = p_val[:, levels:]
        return carry

    lax.fori_loop(0, wave_loc, part_body, 0, unroll=4)
    for b in range(CORES * blocks):
        @pl.when(jnp.logical_not(keeps(b)))
        def _():
            copy_mate(b).start()
    lax.fori_loop(wave_loc, tri_num, part_body, 0, unroll=4)
    for b in range(CORES * blocks):
        @pl.when(keeps(b))
        def _():
            copy_mate(b).wait_recv()

            @pl.loop(0, BLOCK)
            def _(i):
                gap = skip(b)
                for r in range(2):
                    part_own[BLOCK * b + i, r, gap:, :] += part_mate[BLOCK * mate_slot(b) + i, r, gap:, :]

        @pl.when(jnp.logical_and(jnp.logical_and(is_full, chip > 0), core == b % CORES))
        def _():
            copy_part(b).start()

    for c in range(chunks - 1):
        for off in order:
            dst = lax.rem(me + off, group)

            @pl.when(after_parts(dst, c))
            def _():
                copy_b(dst, c, 0, msg, recv_sem_b.at[c]).start()

    for g, start, size in starts(SIZES_B):
        for off in order:
            dst = lax.rem(me + off, group)

            @pl.when(dst < full)
            def _():
                copy_b(dst, chunks - 1, start * SUB, size * SUB, last_sem.at[g]).start()

    for b in range(CORES * blocks):
        @pl.when(jnp.logical_and(chip == 0, core == b % CORES))
        def _():
            gap = skip(b)
            wait_part(b, 0)

            @pl.loop(0, BLOCK)
            def _(i):
                for r in range(2):
                    part_own[BLOCK * b + i, r, gap:, :] += part_in[0, BLOCK * (b % blocks) + i, r, gap:, :]

            copy_part(b).start()

    @pl.when(is_tri)
    def _():
        for c in range(RELAYED):
            for e in range(CORES):
                slot = c * CORES + e
                landed = relay.at[pl.ds(slot * msg, msg)]
                pltpu.make_async_copy(landed, landed, relay_recv.at[slot]).wait()
                copy_onward(c, e).start()

    @pl.when(is_full)
    def _():
        def add_up(m, parts, first):
            re, im = [], []
            for t in range(group * lat_loc // SUB):
                tiles = []
                for q in (2 * t, 2 * t + 1):
                    src, c = divmod(q, chunks)
                    tiles.append(recv_b[rows(((c * group + src) * wave_loc + m) * SUB, SUB), :] if c in parts else None)
                a, b = tiles
                if a is None and b is None:
                    re.append(zero)
                    im.append(zero)
                    continue
                a, b = (zero if x is None else x for x in (a, b))
                re.append(jnp.where(low, a, pltpu.roll(b, QUAD, 0)))
                im.append(jnp.where(low, pltpu.roll(a, QUAD, 0), b))
            h_hi, h_lo = split(jnp.concatenate([jnp.concatenate(re, axis=0), jnp.concatenate(im, axis=0)], axis=1))
            leg_hi, leg_lo = split(leg[m])
            s_val = dot(leg_hi, h_hi) + dot(leg_lo, h_hi) + dot(leg_hi, h_lo)
            for r in range(2):
                value = s_val[:, r * levels:(r + 1) * levels]
                spec[m, r] = value if first else spec[m, r] + value

        for c in range(chunks - 2):
                wait_rows(recv_b, recv_sem_b.at[c], (group - 1) * msg)

        def early_body(m, carry):
            add_up(m, range(chunks - 2), True)
            return carry

        lax.fori_loop(0, wave_loc, early_body, 0, unroll=2)
        wait_rows(recv_b, recv_sem_b.at[chunks - 2], (group - 1) * msg)
        for g, start, size in starts(SIZES_B):
            wait_rows(recv_b, last_sem.at[g], (group - 1) * size * SUB)

            def last_body(i, carry):
                add_up(start + i, (chunks - 2, chunks - 1), False)
                return carry

            lax.fori_loop(0, size, last_body, 0, unroll=2)

    for b in range(CORES * blocks):
        @pl.when(me == full + b // blocks)
        def _():
            gap = skip(b)
            for slot in range(2):
                wait_part(b, slot)

            @pl.loop(0, BLOCK)
            def _(i):
                m = BLOCK * (b % blocks) + i
                for r in range(2):
                    acc = part_own[BLOCK * b + i, r, gap:, :]
                    for slot in range(2):
                        acc = acc + part_in[slot, m, r, gap:, :]
                    spec[m, r, :tri_m + gap, :] = jnp.zeros((tri_m + gap, levels), F32)
                    spec[m, r, tri_m + gap:, :] = acc

    @pl.when(is_full)
    def _():
        wait_rows(send_a, send_sem_a, (group - 1) * chunks * msg)
        wait_rows(send_b, send_sem_b, (full - 1) * chunks * msg)

    @pl.when(is_tri)
    def _():
        wait_rows(send_b, send_sem_b, full * chunks * msg)
        wait_rows(relay, relay_send, RELAYED * CORES * msg)

    for b in range(CORES * blocks):
        @pl.when(jnp.where(is_tri, core == b // blocks, gets(b)))
        def _():
            copy_tri(b, 2, mate).wait_send()

        @pl.when(jnp.logical_and(forwards, gets(b)))
        def _():
            copy_tri(b, 0, mate).wait_send()

        @pl.when(jnp.logical_not(keeps(b)))
        def _():
            copy_mate(b).wait_send()

        @pl.when(me == full + b // blocks)
        def _():
            for lane in range(2):
                copy_tri(b, lane, mate).wait_send()

        @pl.when(jnp.logical_and(is_full, core == b % CORES))
        def _():
            copy_part(b).wait_send()


def solution(mesh):
    group = mesh.shape['w']

    def per_device(coef, legendre, gauss_weight):
        wave_loc, _, levels, degs = coef.shape
        waves = wave_loc * group
        lon = 2 * waves
        lat_loc = legendre.shape[2] // group
        coef_t = jnp.transpose(coef, (0, 1, 3, 2))
        inv, fwd = (jnp.asarray(x) for x in fourier_matrices(waves))
        tri_num = CORES * wave_loc
        tri_deg = degs - waves + tri_num
        blocks = tri_num // BLOCK
        total = group * lat_loc // QUAD * wave_loc * SUB
        dims = (group, wave_loc, levels, degs, lat_loc, waves, lon)
        hbm = pl.BlockSpec(memory_space=pl.ANY)
        vmem = pl.BlockSpec(memory_space=pltpu.VMEM)
        dma = pltpu.SemaphoreType.DMA
        grid, spec = pl.pallas_call(
            functools.partial(kernel, dims),
            out_shape=(pltpu.VMEM((lat_loc, lon, levels), F32), pltpu.VMEM(coef_t.shape, F32)),
            in_specs=[hbm, hbm, hbm, hbm, pl.BlockSpec(memory_space=pltpu.SMEM)],
            out_specs=(vmem, vmem),
            scratch_shapes=[
                pltpu.VMEM(coef_t.shape, F32),
                pltpu.VMEM((wave_loc, degs, legendre.shape[2]), F32),
                pltpu.VMEM(inv.shape, BF16),
                pltpu.VMEM(fwd.shape, BF16),
                pltpu.VMEM((total, levels), F32),
                pltpu.VMEM((total, levels), F32),
                pltpu.VMEM((total, levels), F32),
                pltpu.VMEM((total, levels), F32),
                pltpu.VMEM((tri_num, 2, tri_deg, levels), F32),
                pltpu.VMEM((tri_num, tri_deg, legendre.shape[2]), F32),
                pltpu.VMEM((2, tri_num, OWN, tri_deg), BF16),
                pltpu.VMEM((2, tri_num, tri_deg, OWN), BF16),
                pltpu.VMEM((tri_num, 2, tri_deg, levels), F32),
                pltpu.VMEM((wave_loc, 2, tri_deg, levels), F32),
                pltpu.VMEM((2, wave_loc, 2, tri_deg, levels), F32),
                pltpu.VMEM((RELAYED * CORES * wave_loc * SUB, levels), F32),
                dma((2, len(SIZES_A))), dma((3,)), dma, dma((lat_loc // QUAD,)), dma, dma((lat_loc // QUAD,)), dma((len(SIZES_B),)),
                dma((blocks,)), dma((3, blocks)), dma((blocks,)), dma((blocks,)), dma((blocks,)),
                dma((blocks,)), dma((2, blocks)), dma, dma((RELAYED * CORES,)),
            ],
            compiler_params=pltpu.CompilerParams(collective_id=0, has_side_effects=True, vmem_limit_bytes=48 * 2**20),
            name='transform_pair',
        )(coef_t, legendre, inv, fwd, gauss_weight)
        return jnp.transpose(grid, (2, 0, 1)), jnp.transpose(spec, (0, 1, 3, 2))

    return jax.shard_map(per_device, mesh=mesh, in_specs=(P('w', None, 'lev', None), P(None, None, None), P(None)), out_specs=(P('lev', 'w', None), P('w', None, 'lev', None)), check_vma=False)
```

```python
import functools

import jax
import jax.numpy as jnp
import ml_dtypes
import numpy as np
from jax import lax
from jax.experimental import pallas as pl
from jax.experimental.pallas import tpu as pltpu
from jax.sharding import PartitionSpec as P

MESH = pl.DeviceIdType.MESH
F32, BF16 = jnp.float32, jnp.bfloat16
SUB = 8
QUAD = 4
SIZES_A = (4, 4, 4, 8)
EARLY = 2
SIZES_B = (8, 6, 4, 2)
CORES = 2
BLOCK = 4
PIECES = 5
OWN = 32
HELD = 2
LAG = 2
RELAYED = 2


def split_np(mat):
    hi = mat.astype(np.float32).astype(ml_dtypes.bfloat16)
    lo = (mat - hi.astype(np.float64)).astype(np.float32).astype(ml_dtypes.bfloat16)
    return hi, lo


def fourier_matrices(waves):
    lon = 2 * waves
    m = np.arange(waves)[:, None]
    n = np.arange(lon)[None, :]
    ang = 2.0 * np.pi * ((m * n) % lon) / lon
    fwd = np.concatenate([np.cos(ang), -np.sin(ang)], axis=0)
    scale = np.where(np.arange(waves) == 0, 1.0, 2.0) / lon
    inv = (fwd * np.tile(scale, 2)[:, None]).T
    out = []
    for mat in (inv, fwd):
        hi, lo = split_np(mat)
        out.append(np.concatenate([hi, hi, lo], axis=1))
    return out


def latitude_picks(group, lat_loc, first, num):
    row = np.arange(group * lat_loc)
    col = ((np.arange(group) * lat_loc)[None, :, None] + ((first + np.arange(num)) * QUAD)[:, None, None] + np.arange(QUAD)).reshape(-1)
    one = (row[:, None] == col[None, :]).astype(ml_dtypes.bfloat16)
    none = np.zeros_like(one)
    return np.stack([np.concatenate([one, one, none], axis=1), np.concatenate([none, none, one], axis=1)])


def split(x):
    hi = x.astype(BF16)
    lo = (x - hi.astype(F32)).astype(BF16)
    return hi, lo


def dot(a, b, dims=((1,), (0,))):
    return lax.dot_general(a, b, (dims, ((), ())), preferred_element_type=F32)


def sums(recv, mine, m, parts, group, wave_loc, levels):
    low = lax.broadcasted_iota(jnp.int32, (SUB, levels), 0) < QUAD
    re, im = [], []
    for c in parts:
        for src in range(0, group, 2):
            a, b = (recv[pl.ds(pl.multiple_of(((c * group + src + u) * wave_loc + m) * SUB, SUB), SUB), :] for u in range(2))
            re.append(jnp.where(low, a, pltpu.roll(b, QUAD, 0)))
            im.append(jnp.where(low, pltpu.roll(a, QUAD, 0), b))
    h_hi, h_lo = split(jnp.concatenate([jnp.concatenate(re, axis=0), jnp.concatenate(im, axis=0)], axis=1))
    return dot(mine, jnp.concatenate([h_hi, h_lo, h_hi], axis=0))


def kernel(dims, coef_hbm, leg_hbm, inv_hbm, fwd_hbm, pick_early_hbm, pick_last_hbm, wt_ref, grid, spec, recv_b, leg_last,
           coef, leg, inv, fwd, send_a, recv_a, send_b,
           tri, leg_tri, leg_own, leg_own_t, part_own, part_mate, part_in, relay, pick_early, pick_last, leg_early,
           load_sem, mat_sem, send_sem_a, recv_sem_a, send_sem_b, recv_sem_b, last_sem,
           tri_load, tri_send, tri_recv, mate_send, mate_recv, part_send, part_recv, relay_send, relay_recv):
    group, wave_loc, levels, degs, lat_loc, waves, lon = dims
    chunks = lat_loc // QUAD
    msg = wave_loc * SUB
    chips = group // CORES
    tri_num = CORES * wave_loc
    tri_m = waves - tri_num
    tri_deg = degs - tri_m
    full = group - CORES
    blocks = wave_loc // BLOCK
    me = lax.axis_index('w')
    core = lax.rem(me, CORES)
    chip = lax.div(me, CORES)
    mate = me + 1 - 2 * core
    is_full = me < full
    is_tri = me >= full
    forwards = chip == chips - 2

    def starts(sizes):
        return [(g, sum(sizes[:g]), size) for g, size in enumerate(sizes)]

    def rows(start, size):
        return pl.ds(pl.multiple_of(start, SUB), size)

    def skip(b):
        return BLOCK * b // SUB * SUB

    for m in range(tri_num):
        gap = skip(m // BLOCK)
        if gap:
            for r in range(2):
                tri[m, r, 0:gap, :] = jnp.zeros((gap, levels), F32)

    barrier = pltpu.get_barrier_semaphore()
    for off in range(1, group):
        pl.semaphore_signal(barrier, inc=1, device_id={'w': lax.rem(me + off, group)}, device_id_type=MESH)

    def load_pair(g, start, size):
        own = pl.ds(start, size)
        return (pltpu.make_async_copy(coef_hbm.at[own], coef.at[own], load_sem.at[0, g]),
                pltpu.make_async_copy(leg_hbm.at[pl.ds(me * wave_loc + start, size)], leg.at[own], load_sem.at[1, g]))

    def load_block(b):
        gap = skip(b)
        return pltpu.make_async_copy(
            coef_hbm.at[pl.ds(BLOCK * (b % blocks), BLOCK), :, pl.ds(tri_m + gap, tri_deg - gap), :],
            tri.at[pl.ds(BLOCK * b, BLOCK), :, pl.ds(gap, tri_deg - gap), :], tri_load.at[b])

    @pl.when(is_full)
    def _():
        for args in starts(SIZES_A):
            for copy in load_pair(*args):
                copy.start()

    for b in range(CORES * blocks):
        @pl.when(me == full + b // blocks)
        def _():
            load_block(b).start()

    leg_tri_copy = pltpu.make_async_copy(leg_hbm.at[pl.ds(tri_m, tri_num), pl.ds(tri_m, tri_deg), :], leg_tri, mat_sem.at[2])
    mats = [leg_tri_copy, pltpu.make_async_copy(inv_hbm, inv, mat_sem.at[0]), pltpu.make_async_copy(fwd_hbm, fwd, mat_sem.at[1]),
            pltpu.make_async_copy(pick_early_hbm, pick_early, mat_sem.at[3]), pltpu.make_async_copy(pick_last_hbm, pick_last, mat_sem.at[4])]
    for copy in mats:
        copy.start()

    low = lax.broadcasted_iota(jnp.int32, (SUB, levels), 0) < QUAD

    def copy_a(off, c, start, size):
        dst = lax.rem(me + off, group)
        return pltpu.make_async_remote_copy(
            src_ref=send_a.at[rows((dst * chunks + c) * msg + start, size)],
            dst_ref=recv_a.at[rows((c * group + me) * msg + start, size)],
            send_sem=send_sem_a, recv_sem=recv_sem_a.at[c], device_id={'w': dst}, device_id_type=MESH)

    def copy_b(dst, c, start, size, sem):
        return pltpu.make_async_remote_copy(
            src_ref=send_b.at[rows((c * group + dst) * msg + start, size)],
            dst_ref=recv_b.at[rows((c * group + me) * msg + start, size)],
            send_sem=send_sem_b, recv_sem=sem, device_id={'w': dst}, device_id_type=MESH)

    def after_parts(dst, c):
        return jnp.logical_and(jnp.logical_and(chip == 1, dst < CORES), c >= HELD)

    def copy_relay(dst, c):
        slot = c * CORES + lax.rem(dst, CORES)
        return pltpu.make_async_remote_copy(
            src_ref=send_b.at[rows((c * group + dst) * msg, msg)], dst_ref=relay.at[rows(slot * msg, msg)],
            send_sem=send_sem_b, recv_sem=relay_recv.at[slot], device_id={'w': full + core}, device_id_type=MESH)

    def copy_onward(c, e):
        slot = c * CORES + e
        return pltpu.make_async_remote_copy(
            src_ref=relay.at[rows(slot * msg, msg)], dst_ref=recv_b.at[rows((c * group + core) * msg, msg)],
            send_sem=relay_send, recv_sem=recv_sem_b.at[c], device_id={'w': group // 2 + e}, device_id_type=MESH)

    def copy_tri(b, lane, dst):
        gap = skip(b)
        ref = tri.at[pl.ds(BLOCK * b, BLOCK), :, pl.ds(gap, tri_deg - gap), :]
        return pltpu.make_async_remote_copy(
            src_ref=ref, dst_ref=ref, send_sem=tri_send.at[lane, b], recv_sem=tri_recv.at[b],
            device_id={'w': dst}, device_id_type=MESH)

    def entry(b, at):
        return (b // CORES if at == 1 else b) % CORES

    def gets(b):
        return jnp.where(chip == 1, entry(b, 1), entry(b, 0)) == core

    def keeps(b):
        return jnp.where(is_tri, b // blocks, b % CORES) == core

    def mate_slot(b):
        return jnp.where(is_tri, b % blocks, b // CORES)

    def copy_mate(b):
        gap = skip(b)
        return pltpu.make_async_remote_copy(
            src_ref=part_own.at[pl.ds(BLOCK * b, BLOCK), :, pl.ds(gap, tri_deg - gap), :],
            dst_ref=part_mate.at[pl.ds(BLOCK * mate_slot(b), BLOCK), :, pl.ds(gap, tri_deg - gap), :],
            send_sem=mate_send.at[b], recv_sem=mate_recv.at[b], device_id={'w': mate}, device_id_type=MESH)

    def copy_part(b):
        gap = skip(b)
        to_first = chip == 1
        slot = jnp.where(chip == chips - 2, 1, 0)
        dst = jnp.where(to_first, core, full + b // blocks)
        return pltpu.make_async_remote_copy(
            src_ref=part_own.at[pl.ds(BLOCK * b, BLOCK), :, pl.ds(gap, tri_deg - gap), :],
            dst_ref=part_in.at[slot, pl.ds(BLOCK * (b % blocks), BLOCK), :, pl.ds(gap, tri_deg - gap), :],
            send_sem=part_send.at[b], recv_sem=part_recv.at[slot, b], device_id={'w': dst}, device_id_type=MESH)

    def wait_part(b, slot):
        gap = skip(b)
        landed = part_in.at[slot, pl.ds(BLOCK * (b % blocks), BLOCK), :, pl.ds(gap, tri_deg - gap), :]
        pltpu.make_async_copy(landed, landed, part_recv.at[slot, b]).wait()

    def wait_rows(ref, sem, count):
        landed = ref.at[pl.ds(0, count)]
        pltpu.make_async_copy(landed, landed, sem).wait()

    order = [group // 2, 2, group - 2, group // 2 + 1, 3, group - 1, 1]
    order = order if sorted(order) == list(range(1, group)) else list(range(1, group))

    def held(off, c):
        dst_chip = lax.div(lax.rem(me + off, group), CORES)
        return jnp.logical_and(forwards, jnp.logical_or(dst_chip == 0, jnp.logical_and(dst_chip == 1, c >= HELD)))

    @pl.when(is_full)
    def _():
        for g, start, size in starts(SIZES_A):
            for copy in load_pair(g, start, size):
                copy.wait()

            def legendre_body(i, carry):
                m = start + i
                leg_hi, leg_lo = split(jnp.transpose(leg[m]))
                c_hi, c_lo = split(jnp.concatenate([coef[m, 0], coef[m, 1]], axis=1))
                f = dot(leg_hi, c_hi) + dot(leg_lo, c_hi) + dot(leg_hi, c_lo)
                for t in range(group * lat_loc // SUB):
                    re = f[t * SUB:(t + 1) * SUB, :levels]
                    im = f[t * SUB:(t + 1) * SUB, levels:]
                    send_a[rows((2 * t * wave_loc + m) * SUB, SUB), :] = jnp.where(low, re, pltpu.roll(im, QUAD, 0))
                    send_a[rows(((2 * t + 1) * wave_loc + m) * SUB, SUB), :] = jnp.where(low, pltpu.roll(re, QUAD, 0), im)
                return carry

            lax.fori_loop(0, size, legendre_body, 0, unroll=4)
            if g == 0:
                pl.semaphore_wait(barrier, group - 1)
            for off in order:
                copy_a(off, 0, start * SUB, size * SUB).start()
            if g < EARLY:
                for off in order:
                    @pl.when(jnp.logical_not(held(off, 1)))
                    def _():
                        copy_a(off, 1, start * SUB, size * SUB).start()

        rest = sum(SIZES_A[:EARLY])
        for off in order:
            @pl.when(jnp.logical_not(held(off, 1)))
            def _():
                copy_a(off, 1, rest * SUB, (wave_loc - rest) * SUB).start()

        @pl.loop(2, chunks)
        def _(c):
            for off in order:
                @pl.when(jnp.logical_not(held(off, c)))
                def _():
                    copy_a(off, c, 0, msg).start()

        @pl.loop(0, chunks)
        def _(c):
            recv_a[rows((c * group + me) * msg, msg), :] = send_a[rows((me * chunks + c) * msg, msg), :]

    @pl.when(is_tri)
    def _():
        pl.semaphore_wait(barrier, group - 1)
        for b in range(CORES * blocks):
            @pl.when(core == b // blocks)
            def _():
                load_block(b).wait()
                for lane, dst in enumerate([full - CORES + entry(b, chips - 2), entry(b, 0), mate]):
                    copy_tri(b, lane, dst).start()

    @pl.when(forwards)
    def _():
        for b in range(CORES * blocks):
            @pl.when(gets(b))
            def _():
                copy_tri(b, 2, mate).wait_recv()
                copy_tri(b, 0, full - 2 * CORES + entry(b, 1)).start()
                copy_tri(b, 2, mate).start()

        @pl.loop(1, chunks)
        def _(c):
            for off in order:
                @pl.when(held(off, c))
                def _():
                    copy_a(off, c, 0, msg).start()

    leg_tri_copy.wait()
    lat_all = group * lat_loc

    pick = lax.broadcasted_iota(jnp.int32, (lat_all, OWN), 0) == lax.broadcasted_iota(jnp.int32, (lat_all, OWN), 1) + me * lat_loc
    pick = jnp.logical_and(pick, lax.broadcasted_iota(jnp.int32, (lat_all, OWN), 1) < lat_loc)
    pick = jnp.where(pick, 1.0, 0.0).astype(BF16)

    def own_body(m, carry):
        for half, value in enumerate(split(leg_tri[m])):
            mine = dot(value, pick)
            leg_own_t[half, m] = mine.astype(BF16)
            leg_own[half, m] = jnp.transpose(mine).astype(BF16)
        return carry

    lax.fori_loop(0, tri_num, own_body, 0, unroll=4)

    for b in range(CORES * blocks):
        @pl.when(jnp.logical_and(jnp.logical_and(is_full, jnp.logical_not(forwards)), gets(b)))
        def _():
            copy_tri(b, 2, mate).wait_recv()
            copy_tri(b, 2, mate).start()

    for b in range(CORES * blocks):
        @pl.when(jnp.logical_not(jnp.where(is_tri, core == b // blocks, gets(b))))
        def _():
            copy_tri(b, 2, mate).wait_recv()

    def tri_body(m, carry):
        own_hi, own_lo = leg_own[0, m], leg_own[1, m]
        c_hi, c_lo = split(jnp.concatenate([tri[m, 0], tri[m, 1]], axis=1))
        f = dot(own_hi, c_hi) + dot(own_lo, c_hi) + dot(own_hi, c_lo)
        for c in range(chunks):
            t = c // 2
            re = f[t * SUB:(t + 1) * SUB, :levels]
            im = f[t * SUB:(t + 1) * SUB, levels:]
            tile = jnp.where(low, pltpu.roll(re, QUAD, 0), im) if c % 2 else jnp.where(low, re, pltpu.roll(im, QUAD, 0))
            recv_a[rows(((c * group + full) * wave_loc + m) * SUB, SUB), :] = tile
        return carry

    lax.fori_loop(0, tri_num, tri_body, 0, unroll=4)

    for copy in mats[1:]:
        copy.wait()

    @pl.loop(0, chunks)
    def _(c):
        @pl.when(is_full)
        def _():
            wait_rows(recv_a, recv_sem_a.at[c], (full - 1) * msg)

        @pl.when(is_tri)
        def _():
            wait_rows(recv_a, recv_sem_a.at[c], full * msg)

        @pl.loop(0, QUAD // 2)
        def _(pair):
            halves = []
            for u in range(2):
                row = c * (group * msg) + 2 * pair + u
                re = recv_a[pl.ds(row, waves, stride=SUB), :]
                im = recv_a[pl.ds(row + QUAD, waves, stride=SUB), :]
                halves.append(jnp.concatenate([re, im], axis=0))
            f_hi, f_lo = split(jnp.concatenate(halves, axis=1))
            g_val = dot(inv[...], jnp.concatenate([f_hi, f_lo, f_hi], axis=0))
            for u in range(2):
                grid[c * QUAD + 2 * pair + u] = g_val[:, u * levels:(u + 1) * levels]
            q_hi, q_lo = split(g_val * g_val)
            h = dot(fwd[...], jnp.concatenate([q_hi, q_lo, q_hi], axis=0))
            for u in range(2):
                row = c * (group * msg) + 2 * pair + u
                hw = h[:, u * levels:(u + 1) * levels] * wt_ref[me * lat_loc + c * QUAD + 2 * pair + u]
                send_b[pl.ds(row, waves, stride=SUB), :] = hw[:waves]
                send_b[pl.ds(row + QUAD, waves, stride=SUB), :] = hw[waves:]

        @pl.when(c < chunks - 1)
        def _():
            for off in order:
                dst = lax.rem(me + off, group)
                by_relay = jnp.logical_and(jnp.logical_and(chip == 0, dst >= group // 2), c < RELAYED)

                @pl.when(jnp.logical_and(dst < full, by_relay))
                def _():
                    copy_relay(dst, c).start()

                late = jnp.logical_and(is_tri, lax.div(dst, CORES) == 1)

                ready = jnp.logical_and(jnp.logical_or(jnp.logical_not(late), c >= LAG), jnp.logical_not(after_parts(dst, c)))

                @pl.when(jnp.logical_and(jnp.logical_and(dst < full, jnp.logical_not(by_relay)), ready))
                def _():
                    copy_b(dst, c, 0, msg, recv_sem_b.at[c]).start()

                @pl.when(jnp.logical_and(late, c == LAG))
                def _():
                    for before in range(LAG):
                        copy_b(dst, before, 0, msg, recv_sem_b.at[before]).start()

        @pl.when(is_full)
        def _():
            recv_b[rows((c * group + me) * msg, msg), :] = send_b[rows((c * group + me) * msg, msg), :]

    zero = jnp.zeros((SUB, levels), F32)

    def part_body(i, carry):
        side = jnp.where(i < wave_loc, 1 - core, core)
        spread = BLOCK * (CORES * lax.div(lax.rem(i, wave_loc), BLOCK) + side) + lax.rem(i, BLOCK)
        m = jnp.where(is_tri, lax.rem(i, wave_loc) + side * wave_loc, spread)
        re, im = [], []
        for t in range(OWN // SUB):
            a, b = (send_b[rows((c * waves + tri_m + m) * SUB, SUB), :] if c < chunks else zero for c in (2 * t, 2 * t + 1))
            re.append(jnp.where(low, a, pltpu.roll(b, QUAD, 0)))
            im.append(jnp.where(low, pltpu.roll(a, QUAD, 0), b))
        h_hi, h_lo = split(jnp.concatenate([jnp.concatenate(re, axis=0), jnp.concatenate(im, axis=0)], axis=1))
        own_hi, own_lo = leg_own_t[0, m], leg_own_t[1, m]
        p_val = dot(own_hi, h_hi) + dot(own_lo, h_hi) + dot(own_hi, h_lo)
        part_own[m, 0] = p_val[:, :levels]
        part_own[m, 1] = p_val[:, levels:]
        return carry

    lax.fori_loop(0, wave_loc, part_body, 0, unroll=4)
    for b in range(CORES * blocks):
        @pl.when(jnp.logical_not(keeps(b)))
        def _():
            copy_mate(b).start()
    lax.fori_loop(wave_loc, tri_num, part_body, 0, unroll=4)
    for b in range(CORES * blocks):
        @pl.when(keeps(b))
        def _():
            copy_mate(b).wait_recv()

            @pl.loop(0, BLOCK)
            def _(i):
                gap = skip(b)
                for r in range(2):
                    part_own[BLOCK * b + i, r, gap:, :] += part_mate[BLOCK * mate_slot(b) + i, r, gap:, :]

        @pl.when(jnp.logical_and(jnp.logical_and(is_full, chip > 0), core == b % CORES))
        def _():
            copy_part(b).start()

    for c in range(chunks - 1):
        for off in order:
            dst = lax.rem(me + off, group)

            @pl.when(after_parts(dst, c))
            def _():
                copy_b(dst, c, 0, msg, recv_sem_b.at[c]).start()

    for g, start, size in starts(SIZES_B):
        for off in order:
            dst = lax.rem(me + off, group)

            @pl.when(dst < full)
            def _():
                copy_b(dst, chunks - 1, start * SUB, size * SUB, last_sem.at[g]).start()

    @pl.when(is_full)
    def _():
        def pick_body(m, carry):
            leg_hi, leg_lo = split(leg[m])
            leg_early[m] = (dot(leg_hi, pick_early[0]) + dot(leg_lo, pick_early[1])).astype(BF16)
            leg_last[m] = (dot(leg_hi, pick_last[0]) + dot(leg_lo, pick_last[1])).astype(BF16)
            return carry

        lax.fori_loop(0, wave_loc, pick_body, 0, unroll=2)

    for b in range(CORES * blocks):
        @pl.when(jnp.logical_and(chip == 0, core == b % CORES))
        def _():
            gap = skip(b)
            wait_part(b, 0)

            @pl.loop(0, BLOCK)
            def _(i):
                for r in range(2):
                    part_own[BLOCK * b + i, r, gap:, :] += part_in[0, BLOCK * (b % blocks) + i, r, gap:, :]

            copy_part(b).start()

    @pl.when(is_tri)
    def _():
        for c in range(RELAYED):
            for e in range(CORES):
                slot = c * CORES + e
                landed = relay.at[pl.ds(slot * msg, msg)]
                pltpu.make_async_copy(landed, landed, relay_recv.at[slot]).wait()
                copy_onward(c, e).start()

    @pl.when(is_full)
    def _():
        for c in range(chunks - 2):
                wait_rows(recv_b, recv_sem_b.at[c], (group - 1) * msg)

        def early_body(m, carry):
            s_val = sums(recv_b, leg_early[m], m, range(chunks - 2), group, wave_loc, levels)
            for r in range(2):
                spec[m, r] = s_val[:, r * levels:(r + 1) * levels]
            return carry

        lax.fori_loop(0, wave_loc, early_body, 0, unroll=2)
        wait_rows(recv_b, recv_sem_b.at[chunks - 2], (group - 1) * msg)
        for g, start, size in starts(SIZES_B):
            wait_rows(recv_b, last_sem.at[g], (group - 1) * size * SUB)

    for b in range(CORES * blocks):
        @pl.when(me == full + b // blocks)
        def _():
            gap = skip(b)
            for slot in range(2):
                wait_part(b, slot)

            @pl.loop(0, BLOCK)
            def _(i):
                m = BLOCK * (b % blocks) + i
                for r in range(2):
                    acc = part_own[BLOCK * b + i, r, gap:, :]
                    for slot in range(2):
                        acc = acc + part_in[slot, m, r, gap:, :]
                    spec[m, r, :tri_m + gap, :] = jnp.zeros((tri_m + gap, levels), F32)
                    spec[m, r, tri_m + gap:, :] = acc

    @pl.when(is_full)
    def _():
        wait_rows(send_a, send_sem_a, (group - 1) * chunks * msg)
        wait_rows(send_b, send_sem_b, (full - 1) * chunks * msg)

    @pl.when(is_tri)
    def _():
        wait_rows(send_b, send_sem_b, full * chunks * msg)
        wait_rows(relay, relay_send, RELAYED * CORES * msg)

    for b in range(CORES * blocks):
        @pl.when(jnp.where(is_tri, core == b // blocks, gets(b)))
        def _():
            copy_tri(b, 2, mate).wait_send()

        @pl.when(jnp.logical_and(forwards, gets(b)))
        def _():
            copy_tri(b, 0, mate).wait_send()

        @pl.when(jnp.logical_not(keeps(b)))
        def _():
            copy_mate(b).wait_send()

        @pl.when(me == full + b // blocks)
        def _():
            for lane in range(2):
                copy_tri(b, lane, mate).wait_send()

        @pl.when(jnp.logical_and(is_full, core == b % CORES))
        def _():
            copy_part(b).wait_send()


def finish(dims, grid, early, recv_b, leg_last, grid_hbm, spec_hbm, spec, grid_sem, spec_sem):
    group, wave_loc, levels, degs, lat_loc, waves, lon = dims
    chunks = lat_loc // QUAD
    is_full = lax.axis_index('w') < group - CORES
    copies = []
    for p in range(PIECES):
        part = pl.ds(p * (lat_loc // PIECES), lat_loc // PIECES)
        copies.append(pltpu.make_async_copy(grid.at[part], grid_hbm.at[part], grid_sem.at[p]))
        copies[-1].start()
    size = wave_loc // PIECES
    for p in range(PIECES):
        part = pl.ds(p * size, size)

        @pl.when(is_full)
        def _():
            def last_body(i, carry):
                m = p * size + i
                s_val = sums(recv_b, leg_last[m], m, (chunks - 2, chunks - 1), group, wave_loc, levels)
                for r in range(2):
                    spec[m, r] = early[m, r] + s_val[:, r * levels:(r + 1) * levels]
                return carry

            lax.fori_loop(0, size, last_body, 0, unroll=4)
            pltpu.make_async_copy(spec.at[part], spec_hbm.at[part], spec_sem.at[p]).start()

        @pl.when(jnp.logical_not(is_full))
        def _():
            pltpu.make_async_copy(early.at[part], spec_hbm.at[part], spec_sem.at[p]).start()

        copies.append(pltpu.make_async_copy(spec.at[part], spec_hbm.at[part], spec_sem.at[p]))
    for copy in copies:
        copy.wait()


def solution(mesh):
    group = mesh.shape['w']

    def per_device(coef, legendre, gauss_weight):
        wave_loc, _, levels, degs = coef.shape
        waves = wave_loc * group
        lon = 2 * waves
        lat_loc = legendre.shape[2] // group
        coef_t = jnp.transpose(coef, (0, 1, 3, 2))
        inv, fwd = (jnp.asarray(x) for x in fourier_matrices(waves))
        tri_num = CORES * wave_loc
        tri_deg = degs - waves + tri_num
        blocks = tri_num // BLOCK
        chunks = lat_loc // QUAD
        pick_early = jnp.asarray(latitude_picks(group, lat_loc, 0, chunks - 2))
        pick_last = jnp.asarray(latitude_picks(group, lat_loc, chunks - 2, 2))
        total = group * lat_loc // QUAD * wave_loc * SUB
        dims = (group, wave_loc, levels, degs, lat_loc, waves, lon)
        hbm = pl.BlockSpec(memory_space=pltpu.HBM)
        vmem = pl.BlockSpec(memory_space=pltpu.VMEM)
        dma = pltpu.SemaphoreType.DMA
        grid, spec, recv_b, leg_last = pl.pallas_call(
            functools.partial(kernel, dims),
            out_shape=(pltpu.VMEM((lat_loc, lon, levels), F32), pltpu.VMEM(coef_t.shape, F32), pltpu.VMEM((total, levels), F32), pltpu.VMEM((wave_loc, degs, pick_last.shape[2]), BF16)),
            in_specs=[hbm, hbm, hbm, hbm, hbm, hbm, pl.BlockSpec(memory_space=pltpu.SMEM)],
            out_specs=(vmem, vmem, vmem, vmem),
            scratch_shapes=[
                pltpu.VMEM(coef_t.shape, F32),
                pltpu.VMEM((wave_loc, degs, legendre.shape[2]), F32),
                pltpu.VMEM(inv.shape, BF16),
                pltpu.VMEM(fwd.shape, BF16),
                pltpu.VMEM((total, levels), F32),
                pltpu.VMEM((total, levels), F32),
                pltpu.VMEM((total, levels), F32),
                pltpu.VMEM((tri_num, 2, tri_deg, levels), F32),
                pltpu.VMEM((tri_num, tri_deg, legendre.shape[2]), F32),
                pltpu.VMEM((2, tri_num, OWN, tri_deg), BF16),
                pltpu.VMEM((2, tri_num, tri_deg, OWN), BF16),
                pltpu.VMEM((tri_num, 2, tri_deg, levels), F32),
                pltpu.VMEM((wave_loc, 2, tri_deg, levels), F32),
                pltpu.VMEM((2, wave_loc, 2, tri_deg, levels), F32),
                pltpu.VMEM((RELAYED * CORES * wave_loc * SUB, levels), F32),
                pltpu.VMEM(pick_early.shape, BF16),
                pltpu.VMEM(pick_last.shape, BF16),
                pltpu.VMEM((wave_loc, degs, pick_early.shape[2]), BF16),
                dma((2, len(SIZES_A))), dma((5,)), dma, dma((lat_loc // QUAD,)), dma, dma((lat_loc // QUAD,)), dma((len(SIZES_B),)),
                dma((blocks,)), dma((3, blocks)), dma((blocks,)), dma((blocks,)), dma((blocks,)),
                dma((blocks,)), dma((2, blocks)), dma, dma((RELAYED * CORES,)),
            ],
            compiler_params=pltpu.CompilerParams(collective_id=0, has_side_effects=True, vmem_limit_bytes=52 * 2**20),
            name='transform_pair',
        )(coef_t, legendre, inv, fwd, pick_early, pick_last, gauss_weight)
        grid, spec = pl.pallas_call(
            functools.partial(finish, dims),
            out_shape=(jax.ShapeDtypeStruct(grid.shape, F32), jax.ShapeDtypeStruct(spec.shape, F32)),
            in_specs=[vmem, vmem, vmem, vmem],
            out_specs=(hbm, hbm),
            scratch_shapes=[pltpu.VMEM(spec.shape, F32), dma((PIECES,)), dma((PIECES,))],
            compiler_params=pltpu.CompilerParams(vmem_limit_bytes=8 * 2**20),
            name='finish',
        )(grid, spec, recv_b, leg_last)
        return jnp.transpose(grid, (2, 0, 1)), jnp.transpose(spec, (0, 1, 3, 2))

    return jax.shard_map(per_device, mesh=mesh, in_specs=(P('w', None, 'lev', None), P(None, None, None), P(None)), out_specs=(P('lev', 'w', None), P('w', None, 'lev', None)), check_vma=False)
```

```python
import functools

import jax
import jax.numpy as jnp
import ml_dtypes
import numpy as np
from jax import lax
from jax.experimental import pallas as pl
from jax.experimental.pallas import tpu as pltpu
from jax.sharding import PartitionSpec as P

MESH = pl.DeviceIdType.MESH
F32, BF16 = jnp.float32, jnp.bfloat16
SUB = 8
QUAD = 4
SIZES_A = (2, 6, 4, 8)
EARLY = 2
CORES = 2
BLOCK = 4
PIECES = 5
OWN = 32
HELD = 2
LAG = 2
RELAYED = 2


def split_np(mat):
    hi = mat.astype(np.float32).astype(ml_dtypes.bfloat16)
    lo = (mat - hi.astype(np.float64)).astype(np.float32).astype(ml_dtypes.bfloat16)
    return hi, lo


def fourier_matrices(waves):
    lon = 2 * waves
    m = np.arange(waves)[:, None]
    n = np.arange(lon)[None, :]
    ang = 2.0 * np.pi * ((m * n) % lon) / lon
    fwd = np.concatenate([np.cos(ang), -np.sin(ang)], axis=0)
    scale = np.where(np.arange(waves) == 0, 1.0, 2.0) / lon
    inv = (fwd * np.tile(scale, 2)[:, None]).T
    out = []
    for mat in (inv, fwd):
        hi, lo = split_np(mat)
        out.append(np.concatenate([hi, hi, lo], axis=1))
    return out


def latitude_picks(group, lat_loc, first, num):
    row = np.arange(group * lat_loc)
    col = ((np.arange(group) * lat_loc)[None, :, None] + ((first + np.arange(num)) * QUAD)[:, None, None] + np.arange(QUAD)).reshape(-1)
    one = (row[:, None] == col[None, :]).astype(ml_dtypes.bfloat16)
    none = np.zeros_like(one)
    return np.stack([np.concatenate([one, one, none], axis=1), np.concatenate([none, none, one], axis=1)])


def split(x):
    hi = x.astype(BF16)
    lo = (x - hi.astype(F32)).astype(BF16)
    return hi, lo


def dot(a, b, dims=((1,), (0,))):
    return lax.dot_general(a, b, (dims, ((), ())), preferred_element_type=F32)


def sums(recv, mine, m, parts, group, wave_loc, levels):
    low = lax.broadcasted_iota(jnp.int32, (SUB, levels), 0) < QUAD
    re, im = [], []
    for c in parts:
        for src in range(0, group, 2):
            a, b = (recv[pl.ds(pl.multiple_of(((c * group + src + u) * wave_loc + m) * SUB, SUB), SUB), :] for u in range(2))
            re.append(jnp.where(low, a, pltpu.roll(b, QUAD, 0)))
            im.append(jnp.where(low, pltpu.roll(a, QUAD, 0), b))
    h_hi, h_lo = split(jnp.concatenate([jnp.concatenate(re, axis=0), jnp.concatenate(im, axis=0)], axis=1))
    return dot(mine, jnp.concatenate([h_hi, h_lo, h_hi], axis=0))


def kernel(dims, coef_hbm, leg_hbm, inv_hbm, fwd_hbm, pick_early_hbm, pick_last_hbm, wt_ref, grid, spec, recv_b, leg_last,
           coef, leg, inv, fwd, send_a, recv_a, send_b,
           tri, leg_tri, leg_own, leg_own_t, part_own, part_mate, part_in, relay, pick_early, pick_last, leg_early,
           load_sem, mat_sem, send_sem_a, recv_sem_a, send_sem_b, recv_sem_b,
           tri_load, tri_recv, mate_recv, part_recv, relay_recv, misc_send):
    group, wave_loc, levels, degs, lat_loc, waves, lon = dims
    chunks = lat_loc // QUAD
    msg = wave_loc * SUB
    chips = group // CORES
    tri_num = CORES * wave_loc
    tri_m = waves - tri_num
    tri_deg = degs - tri_m
    full = group - CORES
    blocks = wave_loc // BLOCK
    me = lax.axis_index('w')
    core = lax.rem(me, CORES)
    chip = lax.div(me, CORES)
    mate = me + 1 - 2 * core
    is_full = me < full
    is_tri = me >= full
    forwards = chip == chips - 2

    def starts(sizes):
        return [(g, sum(sizes[:g]), size) for g, size in enumerate(sizes)]

    def rows(start, size):
        return pl.ds(pl.multiple_of(start, SUB), size)

    def skip(b):
        return BLOCK * b // SUB * SUB

    for m in range(tri_num):
        gap = skip(m // BLOCK)
        if gap:
            for r in range(2):
                tri[m, r, 0:gap, :] = jnp.zeros((gap, levels), F32)

    barrier = pltpu.get_barrier_semaphore()
    for off in range(1, group):
        pl.semaphore_signal(barrier, inc=1, device_id={'w': lax.rem(me + off, group)}, device_id_type=MESH)

    def load_pair(g, start, size):
        own = pl.ds(start, size)
        return (pltpu.make_async_copy(coef_hbm.at[own], coef.at[own], load_sem.at[0, g]),
                pltpu.make_async_copy(leg_hbm.at[pl.ds(me * wave_loc + start, size)], leg.at[own], load_sem.at[1, g]))

    def load_block(b):
        gap = skip(b)
        return pltpu.make_async_copy(
            coef_hbm.at[pl.ds(BLOCK * (b % blocks), BLOCK), :, pl.ds(tri_m + gap, tri_deg - gap), :],
            tri.at[pl.ds(BLOCK * b, BLOCK), :, pl.ds(gap, tri_deg - gap), :], tri_load.at[b % blocks])

    @pl.when(is_full)
    def _():
        for args in starts(SIZES_A):
            for copy in load_pair(*args):
                copy.start()

    for b in range(CORES * blocks):
        @pl.when(me == full + b // blocks)
        def _():
            load_block(b).start()

    leg_tri_copy = pltpu.make_async_copy(leg_hbm.at[pl.ds(tri_m, tri_num), pl.ds(tri_m, tri_deg), :], leg_tri, mat_sem.at[2])
    mats = [leg_tri_copy, pltpu.make_async_copy(inv_hbm, inv, mat_sem.at[0]), pltpu.make_async_copy(fwd_hbm, fwd, mat_sem.at[1]),
            pltpu.make_async_copy(pick_early_hbm, pick_early, mat_sem.at[3]), pltpu.make_async_copy(pick_last_hbm, pick_last, mat_sem.at[4])]
    for copy in mats:
        copy.start()

    low = lax.broadcasted_iota(jnp.int32, (SUB, levels), 0) < QUAD

    def copy_a(off, c, start, size):
        dst = lax.rem(me + off, group)
        return pltpu.make_async_remote_copy(
            src_ref=send_a.at[rows((dst * chunks + c) * msg + start, size)],
            dst_ref=recv_a.at[rows((c * group + me) * msg + start, size)],
            send_sem=send_sem_a, recv_sem=recv_sem_a.at[c], device_id={'w': dst}, device_id_type=MESH)

    def copy_b(dst, c, start, size, sem):
        return pltpu.make_async_remote_copy(
            src_ref=send_b.at[rows((c * group + dst) * msg + start, size)],
            dst_ref=recv_b.at[rows((c * group + me) * msg + start, size)],
            send_sem=send_sem_b, recv_sem=sem, device_id={'w': dst}, device_id_type=MESH)

    def after_parts(dst, c):
        return jnp.logical_and(jnp.logical_and(chip == 1, dst < CORES), c >= HELD)

    def copy_relay(dst, c):
        slot = c * CORES + lax.rem(dst, CORES)
        return pltpu.make_async_remote_copy(
            src_ref=send_b.at[rows((c * group + dst) * msg, msg)], dst_ref=relay.at[rows(slot * msg, msg)],
            send_sem=send_sem_b, recv_sem=relay_recv.at[slot], device_id={'w': full + core}, device_id_type=MESH)

    def copy_onward(c, e):
        slot = c * CORES + e
        return pltpu.make_async_remote_copy(
            src_ref=relay.at[rows(slot * msg, msg)], dst_ref=recv_b.at[rows((c * group + core) * msg, msg)],
            send_sem=misc_send, recv_sem=recv_sem_b.at[c], device_id={'w': group // 2 + e}, device_id_type=MESH)

    def copy_tri(b, dst):
        gap = skip(b)
        ref = tri.at[pl.ds(BLOCK * b, BLOCK), :, pl.ds(gap, tri_deg - gap), :]
        return pltpu.make_async_remote_copy(
            src_ref=ref, dst_ref=ref, send_sem=misc_send, recv_sem=tri_recv.at[b],
            device_id={'w': dst}, device_id_type=MESH)

    def entry(b, at):
        return (b // CORES if at == 1 else b) % CORES

    def gets(b):
        return jnp.where(chip == 1, entry(b, 1), entry(b, 0)) == core

    def keeps(b):
        return jnp.where(is_tri, b // blocks, b % CORES) == core

    def mate_slot(b):
        return jnp.where(is_tri, b % blocks, b // CORES)

    def copy_mate(b):
        gap = skip(b)
        return pltpu.make_async_remote_copy(
            src_ref=part_own.at[pl.ds(BLOCK * b, BLOCK), :, pl.ds(gap, tri_deg - gap), :],
            dst_ref=part_mate.at[pl.ds(BLOCK * mate_slot(b), BLOCK), :, pl.ds(gap, tri_deg - gap), :],
            send_sem=misc_send, recv_sem=mate_recv.at[mate_slot(b)], device_id={'w': mate}, device_id_type=MESH)

    def copy_part(b):
        gap = skip(b)
        to_first = chip == 1
        slot = jnp.where(chip == chips - 2, 1, 0)
        dst = jnp.where(to_first, core, full + b // blocks)
        return pltpu.make_async_remote_copy(
            src_ref=part_own.at[pl.ds(BLOCK * b, BLOCK), :, pl.ds(gap, tri_deg - gap), :],
            dst_ref=part_in.at[slot, pl.ds(BLOCK * (b % blocks), BLOCK), :, pl.ds(gap, tri_deg - gap), :],
            send_sem=misc_send, recv_sem=part_recv.at[slot, b % blocks], device_id={'w': dst}, device_id_type=MESH)

    def wait_part(b, slot):
        gap = skip(b)
        landed = part_in.at[slot, pl.ds(BLOCK * (b % blocks), BLOCK), :, pl.ds(gap, tri_deg - gap), :]
        pltpu.make_async_copy(landed, landed, part_recv.at[slot, b % blocks]).wait()

    def wait_rows(ref, sem, count):
        landed = ref.at[pl.ds(0, count)]
        pltpu.make_async_copy(landed, landed, sem).wait()

    order = [group // 2, 2, group - 2, group // 2 + 1, 3, group - 1, 1]
    order = order if sorted(order) == list(range(1, group)) else list(range(1, group))

    def held(off, c):
        dst_chip = lax.div(lax.rem(me + off, group), CORES)
        return jnp.logical_and(jnp.logical_and(forwards, dst_chip == 1), c >= HELD)

    @pl.when(is_full)
    def _():
        for g, start, size in starts(SIZES_A):
            for copy in load_pair(g, start, size):
                copy.wait()

            def legendre_body(i, carry):
                m = start + i
                leg_hi, leg_lo = split(jnp.transpose(leg[m]))
                c_hi, c_lo = split(jnp.concatenate([coef[m, 0], coef[m, 1]], axis=1))
                f = dot(leg_hi, c_hi) + dot(leg_lo, c_hi) + dot(leg_hi, c_lo)
                for t in range(group * lat_loc // SUB):
                    re = f[t * SUB:(t + 1) * SUB, :levels]
                    im = f[t * SUB:(t + 1) * SUB, levels:]
                    send_a[rows((2 * t * wave_loc + m) * SUB, SUB), :] = jnp.where(low, re, pltpu.roll(im, QUAD, 0))
                    send_a[rows(((2 * t + 1) * wave_loc + m) * SUB, SUB), :] = jnp.where(low, pltpu.roll(re, QUAD, 0), im)
                return carry

            lax.fori_loop(0, size, legendre_body, 0, unroll=4)
            if g == 0:
                pl.semaphore_wait(barrier, group - 1)
            for off in order:
                copy_a(off, 0, start * SUB, size * SUB).start()
            if g < EARLY:
                for off in order:
                    @pl.when(jnp.logical_not(held(off, 1)))
                    def _():
                        copy_a(off, 1, start * SUB, size * SUB).start()

        rest = sum(SIZES_A[:EARLY])
        for off in order:
            @pl.when(jnp.logical_not(held(off, 1)))
            def _():
                copy_a(off, 1, rest * SUB, (wave_loc - rest) * SUB).start()

        @pl.loop(2, chunks)
        def _(c):
            for off in order:
                @pl.when(jnp.logical_not(held(off, c)))
                def _():
                    copy_a(off, c, 0, msg).start()

        @pl.loop(0, chunks)
        def _(c):
            recv_a[rows((c * group + me) * msg, msg), :] = send_a[rows((me * chunks + c) * msg, msg), :]

    @pl.when(is_tri)
    def _():
        pl.semaphore_wait(barrier, group - 1)
        for b in range(CORES * blocks):
            @pl.when(core == b // blocks)
            def _():
                load_block(b).wait()
                for dst in (full - CORES + entry(b, chips - 2), entry(b, 0), mate):
                    copy_tri(b, dst).start()

    @pl.when(forwards)
    def _():
        for b in range(CORES * blocks):
            @pl.when(gets(b))
            def _():
                copy_tri(b, mate).wait_recv()
                copy_tri(b, full - 2 * CORES + entry(b, 1)).start()
                copy_tri(b, mate).start()

        @pl.loop(1, chunks)
        def _(c):
            for off in order:
                @pl.when(held(off, c))
                def _():
                    copy_a(off, c, 0, msg).start()

    leg_tri_copy.wait()
    lat_all = group * lat_loc

    pick = lax.broadcasted_iota(jnp.int32, (lat_all, OWN), 0) == lax.broadcasted_iota(jnp.int32, (lat_all, OWN), 1) + me * lat_loc
    pick = jnp.logical_and(pick, lax.broadcasted_iota(jnp.int32, (lat_all, OWN), 1) < lat_loc)
    pick = jnp.where(pick, 1.0, 0.0).astype(BF16)

    def own_body(m, carry):
        for half, value in enumerate(split(leg_tri[m])):
            mine = dot(value, pick)
            leg_own_t[half, m] = mine.astype(BF16)
            leg_own[half, m] = jnp.transpose(mine).astype(BF16)
        return carry

    lax.fori_loop(0, tri_num, own_body, 0, unroll=4)

    for b in range(CORES * blocks):
        @pl.when(jnp.logical_and(jnp.logical_and(is_full, jnp.logical_not(forwards)), gets(b)))
        def _():
            copy_tri(b, mate).wait_recv()
            copy_tri(b, mate).start()

    for b in range(CORES * blocks):
        @pl.when(jnp.logical_not(jnp.where(is_tri, core == b // blocks, gets(b))))
        def _():
            copy_tri(b, mate).wait_recv()

    def tri_body(m, carry):
        own_hi, own_lo = leg_own[0, m], leg_own[1, m]
        c_hi, c_lo = split(jnp.concatenate([tri[m, 0], tri[m, 1]], axis=1))
        f = dot(own_hi, c_hi) + dot(own_lo, c_hi) + dot(own_hi, c_lo)
        for c in range(chunks):
            t = c // 2
            re = f[t * SUB:(t + 1) * SUB, :levels]
            im = f[t * SUB:(t + 1) * SUB, levels:]
            tile = jnp.where(low, pltpu.roll(re, QUAD, 0), im) if c % 2 else jnp.where(low, re, pltpu.roll(im, QUAD, 0))
            recv_a[rows(((c * group + full) * wave_loc + m) * SUB, SUB), :] = tile
        return carry

    lax.fori_loop(0, tri_num, tri_body, 0, unroll=4)

    for copy in mats[1:]:
        copy.wait()

    @pl.loop(0, chunks)
    def _(c):
        @pl.when(is_full)
        def _():
            wait_rows(recv_a, recv_sem_a.at[c], (full - 1) * msg)

        @pl.when(is_tri)
        def _():
            wait_rows(recv_a, recv_sem_a.at[c], full * msg)

        @pl.loop(0, QUAD // 2)
        def _(pair):
            halves = []
            for u in range(2):
                row = c * (group * msg) + 2 * pair + u
                re = recv_a[pl.ds(row, waves, stride=SUB), :]
                im = recv_a[pl.ds(row + QUAD, waves, stride=SUB), :]
                halves.append(jnp.concatenate([re, im], axis=0))
            f_hi, f_lo = split(jnp.concatenate(halves, axis=1))
            g_val = dot(inv[...], jnp.concatenate([f_hi, f_lo, f_hi], axis=0))
            for u in range(2):
                grid[c * QUAD + 2 * pair + u] = g_val[:, u * levels:(u + 1) * levels]
            q_hi, q_lo = split(g_val * g_val)
            h = dot(fwd[...], jnp.concatenate([q_hi, q_lo, q_hi], axis=0))
            for u in range(2):
                row = c * (group * msg) + 2 * pair + u
                hw = h[:, u * levels:(u + 1) * levels] * wt_ref[me * lat_loc + c * QUAD + 2 * pair + u]
                send_b[pl.ds(row, waves, stride=SUB), :] = hw[:waves]
                send_b[pl.ds(row + QUAD, waves, stride=SUB), :] = hw[waves:]

        @pl.when(c < chunks - 1)
        def _():
            for off in order:
                dst = lax.rem(me + off, group)
                by_relay = jnp.logical_and(jnp.logical_and(chip == 0, dst >= group // 2), c < RELAYED)

                @pl.when(jnp.logical_and(dst < full, by_relay))
                def _():
                    copy_relay(dst, c).start()

                late = jnp.logical_and(is_tri, lax.div(dst, CORES) == 1)

                ready = jnp.logical_and(jnp.logical_or(jnp.logical_not(late), c >= LAG), jnp.logical_not(after_parts(dst, c)))

                @pl.when(jnp.logical_and(jnp.logical_and(dst < full, jnp.logical_not(by_relay)), ready))
                def _():
                    copy_b(dst, c, 0, msg, recv_sem_b.at[c]).start()

                @pl.when(jnp.logical_and(late, c == LAG))
                def _():
                    for before in range(LAG):
                        copy_b(dst, before, 0, msg, recv_sem_b.at[before]).start()

        @pl.when(is_full)
        def _():
            recv_b[rows((c * group + me) * msg, msg), :] = send_b[rows((c * group + me) * msg, msg), :]

    zero = jnp.zeros((SUB, levels), F32)

    def part_body(i, carry):
        side = jnp.where(i < wave_loc, 1 - core, core)
        spread = BLOCK * (CORES * lax.div(lax.rem(i, wave_loc), BLOCK) + side) + lax.rem(i, BLOCK)
        m = jnp.where(is_tri, lax.rem(i, wave_loc) + side * wave_loc, spread)
        re, im = [], []
        for t in range(OWN // SUB):
            a, b = (send_b[rows((c * waves + tri_m + m) * SUB, SUB), :] if c < chunks else zero for c in (2 * t, 2 * t + 1))
            re.append(jnp.where(low, a, pltpu.roll(b, QUAD, 0)))
            im.append(jnp.where(low, pltpu.roll(a, QUAD, 0), b))
        h_hi, h_lo = split(jnp.concatenate([jnp.concatenate(re, axis=0), jnp.concatenate(im, axis=0)], axis=1))
        own_hi, own_lo = leg_own_t[0, m], leg_own_t[1, m]
        p_val = dot(own_hi, h_hi) + dot(own_lo, h_hi) + dot(own_hi, h_lo)
        part_own[m, 0] = p_val[:, :levels]
        part_own[m, 1] = p_val[:, levels:]
        return carry

    lax.fori_loop(0, wave_loc, part_body, 0, unroll=4)
    for b in range(CORES * blocks):
        @pl.when(jnp.logical_not(keeps(b)))
        def _():
            copy_mate(b).start()
    lax.fori_loop(wave_loc, tri_num, part_body, 0, unroll=4)
    for b in range(CORES * blocks):
        @pl.when(keeps(b))
        def _():
            copy_mate(b).wait_recv()

            @pl.loop(0, BLOCK)
            def _(i):
                gap = skip(b)
                for r in range(2):
                    part_own[BLOCK * b + i, r, gap:, :] += part_mate[BLOCK * mate_slot(b) + i, r, gap:, :]

        @pl.when(jnp.logical_and(jnp.logical_and(is_full, chip > 0), core == b % CORES))
        def _():
            copy_part(b).start()

    for c in range(chunks - 1):
        for off in order:
            dst = lax.rem(me + off, group)

            @pl.when(after_parts(dst, c))
            def _():
                copy_b(dst, c, 0, msg, recv_sem_b.at[c]).start()

    for off in order:
        dst = lax.rem(me + off, group)

        @pl.when(dst < full)
        def _():
            copy_b(dst, chunks - 1, 0, msg, recv_sem_b.at[chunks - 1]).start()

    @pl.when(is_full)
    def _():
        def pick_body(m, carry):
            leg_hi, leg_lo = split(leg[m])
            leg_early[m] = (dot(leg_hi, pick_early[0]) + dot(leg_lo, pick_early[1])).astype(BF16)
            leg_last[m] = (dot(leg_hi, pick_last[0]) + dot(leg_lo, pick_last[1])).astype(BF16)
            return carry

        lax.fori_loop(0, wave_loc, pick_body, 0, unroll=2)

    for b in range(CORES * blocks):
        @pl.when(jnp.logical_and(chip == 0, core == b % CORES))
        def _():
            gap = skip(b)
            wait_part(b, 0)

            @pl.loop(0, BLOCK)
            def _(i):
                for r in range(2):
                    part_own[BLOCK * b + i, r, gap:, :] += part_in[0, BLOCK * (b % blocks) + i, r, gap:, :]

            copy_part(b).start()

    @pl.when(is_tri)
    def _():
        for c in range(RELAYED):
            for e in range(CORES):
                slot = c * CORES + e
                landed = relay.at[pl.ds(slot * msg, msg)]
                pltpu.make_async_copy(landed, landed, relay_recv.at[slot]).wait()
                copy_onward(c, e).start()

    @pl.when(is_full)
    def _():
        for c in range(chunks - 2):
                wait_rows(recv_b, recv_sem_b.at[c], (group - 1) * msg)

        def early_body(m, carry):
            s_val = sums(recv_b, leg_early[m], m, range(chunks - 2), group, wave_loc, levels)
            for r in range(2):
                spec[m, r] = s_val[:, r * levels:(r + 1) * levels]
            return carry

        lax.fori_loop(0, wave_loc, early_body, 0, unroll=2)
        for c in range(chunks - 2, chunks):
            wait_rows(recv_b, recv_sem_b.at[c], (group - 1) * msg)

    for b in range(CORES * blocks):
        @pl.when(me == full + b // blocks)
        def _():
            gap = skip(b)
            for slot in range(2):
                wait_part(b, slot)

            @pl.loop(0, BLOCK)
            def _(i):
                m = BLOCK * (b % blocks) + i
                for r in range(2):
                    acc = part_own[BLOCK * b + i, r, gap:, :]
                    for slot in range(2):
                        acc = acc + part_in[slot, m, r, gap:, :]
                    spec[m, r, :tri_m + gap, :] = jnp.zeros((tri_m + gap, levels), F32)
                    spec[m, r, tri_m + gap:, :] = acc

    @pl.when(is_full)
    def _():
        wait_rows(send_a, send_sem_a, (group - 1) * chunks * msg)
        wait_rows(send_b, send_sem_b, (full - 1) * chunks * msg)

    @pl.when(is_tri)
    def _():
        wait_rows(send_b, send_sem_b, full * chunks * msg)

    def block_rows(blks):
        return sum(BLOCK * 2 * (tri_deg - skip(b)) for b in blks)

    for at in range(chips):
        for p in range(CORES):
            if at == chips - 1:
                own = [b for b in range(CORES * blocks) if b // blocks == p]
                mates = [b for b in range(CORES * blocks) if b // blocks != p]
                count = 3 * block_rows(own) + block_rows(mates) + RELAYED * CORES * msg
            else:
                come = [b for b in range(CORES * blocks) if entry(b, at) == p]
                count = block_rows(come) * (2 if at == chips - 2 else 1) + block_rows(range(CORES * blocks))

            @pl.when(jnp.logical_and(chip == at, core == p))
            def _():
                wait_rows(send_a, misc_send, count)


def finish(dims, grid, early, recv_b, leg_last, grid_hbm, spec_hbm, spec, grid_sem, spec_sem):
    group, wave_loc, levels, degs, lat_loc, waves, lon = dims
    chunks = lat_loc // QUAD
    is_full = lax.axis_index('w') < group - CORES
    copies = []
    for p in range(PIECES):
        part = pl.ds(p * (lat_loc // PIECES), lat_loc // PIECES)
        copies.append(pltpu.make_async_copy(grid.at[part], grid_hbm.at[part], grid_sem.at[p]))
        copies[-1].start()
    size = wave_loc // PIECES
    for p in range(PIECES):
        part = pl.ds(p * size, size)

        @pl.when(is_full)
        def _():
            def last_body(i, carry):
                m = p * size + i
                s_val = sums(recv_b, leg_last[m], m, (chunks - 2, chunks - 1), group, wave_loc, levels)
                for r in range(2):
                    spec[m, r] = early[m, r] + s_val[:, r * levels:(r + 1) * levels]
                return carry

            lax.fori_loop(0, size, last_body, 0, unroll=4)
            pltpu.make_async_copy(spec.at[part], spec_hbm.at[part], spec_sem.at[p]).start()

        @pl.when(jnp.logical_not(is_full))
        def _():
            pltpu.make_async_copy(early.at[part], spec_hbm.at[part], spec_sem.at[p]).start()

        copies.append(pltpu.make_async_copy(spec.at[part], spec_hbm.at[part], spec_sem.at[p]))
    for copy in copies:
        copy.wait()


def solution(mesh):
    group = mesh.shape['w']

    def per_device(coef, legendre, gauss_weight):
        wave_loc, _, levels, degs = coef.shape
        waves = wave_loc * group
        lon = 2 * waves
        lat_loc = legendre.shape[2] // group
        coef_t = jnp.transpose(coef, (0, 1, 3, 2))
        inv, fwd = (jnp.asarray(x) for x in fourier_matrices(waves))
        tri_num = CORES * wave_loc
        tri_deg = degs - waves + tri_num
        blocks = tri_num // BLOCK
        chunks = lat_loc // QUAD
        pick_early = jnp.asarray(latitude_picks(group, lat_loc, 0, chunks - 2))
        pick_last = jnp.asarray(latitude_picks(group, lat_loc, chunks - 2, 2))
        total = group * lat_loc // QUAD * wave_loc * SUB
        dims = (group, wave_loc, levels, degs, lat_loc, waves, lon)
        hbm = pl.BlockSpec(memory_space=pltpu.HBM)
        vmem = pl.BlockSpec(memory_space=pltpu.VMEM)
        dma = pltpu.SemaphoreType.DMA
        grid, spec, recv_b, leg_last = pl.pallas_call(
            functools.partial(kernel, dims),
            out_shape=(pltpu.VMEM((lat_loc, lon, levels), F32), pltpu.VMEM(coef_t.shape, F32), pltpu.VMEM((total, levels), F32), pltpu.VMEM((wave_loc, degs, pick_last.shape[2]), BF16)),
            in_specs=[hbm, hbm, hbm, hbm, hbm, hbm, pl.BlockSpec(memory_space=pltpu.SMEM)],
            out_specs=(vmem, vmem, vmem, vmem),
            scratch_shapes=[
                pltpu.VMEM(coef_t.shape, F32),
                pltpu.VMEM((wave_loc, degs, legendre.shape[2]), F32),
                pltpu.VMEM(inv.shape, BF16),
                pltpu.VMEM(fwd.shape, BF16),
                pltpu.VMEM((total, levels), F32),
                pltpu.VMEM((total, levels), F32),
                pltpu.VMEM((total, levels), F32),
                pltpu.VMEM((tri_num, 2, tri_deg, levels), F32),
                pltpu.VMEM((tri_num, tri_deg, legendre.shape[2]), F32),
                pltpu.VMEM((2, tri_num, OWN, tri_deg), BF16),
                pltpu.VMEM((2, tri_num, tri_deg, OWN), BF16),
                pltpu.VMEM((tri_num, 2, tri_deg, levels), F32),
                pltpu.VMEM((wave_loc, 2, tri_deg, levels), F32),
                pltpu.VMEM((2, wave_loc, 2, tri_deg, levels), F32),
                pltpu.VMEM((RELAYED * CORES * wave_loc * SUB, levels), F32),
                pltpu.VMEM(pick_early.shape, BF16),
                pltpu.VMEM(pick_last.shape, BF16),
                pltpu.VMEM((wave_loc, degs, pick_early.shape[2]), BF16),
                dma((2, len(SIZES_A))), dma((5,)), dma, dma((lat_loc // QUAD,)), dma, dma((lat_loc // QUAD,)),
                dma((blocks // CORES,)), dma((blocks,)), dma((blocks // CORES,)), dma((2, blocks // CORES)), dma((RELAYED * CORES,)), dma,
            ],
            compiler_params=pltpu.CompilerParams(collective_id=0, has_side_effects=True, vmem_limit_bytes=52 * 2**20),
            name='transform_pair',
        )(coef_t, legendre, inv, fwd, pick_early, pick_last, gauss_weight)
        grid, spec = pl.pallas_call(
            functools.partial(finish, dims),
            out_shape=(jax.ShapeDtypeStruct(grid.shape, F32), jax.ShapeDtypeStruct(spec.shape, F32)),
            in_specs=[vmem, vmem, vmem, vmem],
            out_specs=(hbm, hbm),
            scratch_shapes=[pltpu.VMEM(spec.shape, F32), dma((PIECES,)), dma((PIECES,))],
            compiler_params=pltpu.CompilerParams(vmem_limit_bytes=8 * 2**20),
            name='finish',
        )(grid, spec, recv_b, leg_last)
        return jnp.transpose(grid, (2, 0, 1)), jnp.transpose(spec, (0, 1, 3, 2))

    return jax.shard_map(per_device, mesh=mesh, in_specs=(P('w', None, 'lev', None), P(None, None, None), P(None)), out_specs=(P('lev', 'w', None), P('w', None, 'lev', None)), check_vma=False)
```

```python
import functools

import jax
import jax.numpy as jnp
import ml_dtypes
import numpy as np
from jax import lax
from jax.experimental import pallas as pl
from jax.experimental.pallas import tpu as pltpu
from jax.sharding import PartitionSpec as P

MESH = pl.DeviceIdType.MESH
F32, BF16 = jnp.float32, jnp.bfloat16
SUB = 8
QUAD = 4
SIZES_A = (2, 6, 4, 8)
EARLY = 2
CORES = 2
BLOCK = 4
PIECES = 5
OWN = 32
HELD = 2
LAG = 2
RELAYED = 2


def split_np(mat):
    hi = mat.astype(np.float32).astype(ml_dtypes.bfloat16)
    lo = (mat - hi.astype(np.float64)).astype(np.float32).astype(ml_dtypes.bfloat16)
    return hi, lo


def fourier_matrices(waves):
    lon = 2 * waves
    m = np.arange(waves)[:, None]
    n = np.arange(lon)[None, :]
    ang = 2.0 * np.pi * ((m * n) % lon) / lon
    fwd = np.concatenate([np.cos(ang), -np.sin(ang)], axis=0)
    scale = np.where(np.arange(waves) == 0, 1.0, 2.0) / lon
    inv = (fwd * np.tile(scale, 2)[:, None]).T
    out = []
    for mat in (inv, fwd):
        hi, lo = split_np(mat)
        out.append(np.concatenate([hi, hi, lo], axis=1))
    return out


def latitude_picks(group, lat_loc, first, num):
    row = np.arange(group * lat_loc)
    col = ((np.arange(group) * lat_loc)[None, :, None] + ((first + np.arange(num)) * QUAD)[:, None, None] + np.arange(QUAD)).reshape(-1)
    one = (row[:, None] == col[None, :]).astype(ml_dtypes.bfloat16)
    none = np.zeros_like(one)
    return np.stack([np.concatenate([one, one, none], axis=1), np.concatenate([none, none, one], axis=1)])


def split(x):
    hi = x.astype(BF16)
    lo = (x - hi.astype(F32)).astype(BF16)
    return hi, lo


def dot(a, b, dims=((1,), (0,))):
    return lax.dot_general(a, b, (dims, ((), ())), preferred_element_type=F32)


def sums(recv, mine, m, parts, group, wave_loc, levels):
    low = lax.broadcasted_iota(jnp.int32, (SUB, levels), 0) < QUAD
    re, im = [], []
    for c in parts:
        for src in range(0, group, 2):
            a, b = (recv[pl.ds(pl.multiple_of(((c * group + src + u) * wave_loc + m) * SUB, SUB), SUB), :] for u in range(2))
            re.append(jnp.where(low, a, pltpu.roll(b, QUAD, 0)))
            im.append(jnp.where(low, pltpu.roll(a, QUAD, 0), b))
    h_hi, h_lo = split(jnp.concatenate([jnp.concatenate(re, axis=0), jnp.concatenate(im, axis=0)], axis=1))
    return dot(mine, jnp.concatenate([h_hi, h_lo, h_hi], axis=0))


def kernel(dims, coef_hbm, leg_hbm, inv_hbm, fwd_hbm, pick_early_hbm, pick_last_hbm, wt_ref, grid, spec, recv_b, leg_last,
           coef, leg, inv, fwd, send_a, recv_a, send_b,
           tri, leg_tri, leg_own, leg_own_t, part_own, part_mate, part_in, relay, pick_early, pick_last, leg_early,
           load_sem, mat_sem, send_sem_a, recv_sem_a, send_sem_b, recv_sem_b,
           tri_recv, mate_recv, part_recv, misc_send):
    group, wave_loc, levels, degs, lat_loc, waves, lon = dims
    chunks = lat_loc // QUAD
    msg = wave_loc * SUB
    chips = group // CORES
    tri_num = CORES * wave_loc
    tri_m = waves - tri_num
    tri_deg = degs - tri_m
    full = group - CORES
    blocks = wave_loc // BLOCK
    me = lax.axis_index('w')
    core = lax.rem(me, CORES)
    chip = lax.div(me, CORES)
    mate = me + 1 - 2 * core
    is_full = me < full
    is_tri = me >= full
    forwards = chip == chips - 2

    def starts(sizes):
        return [(g, sum(sizes[:g]), size) for g, size in enumerate(sizes)]

    def rows(start, size):
        return pl.ds(pl.multiple_of(start, SUB), size)

    def skip(b):
        return BLOCK * b // SUB * SUB

    for m in range(tri_num):
        gap = skip(m // BLOCK)
        if gap:
            for r in range(2):
                tri[m, r, 0:gap, :] = jnp.zeros((gap, levels), F32)

    barrier = pltpu.get_barrier_semaphore()
    for off in range(1, group):
        pl.semaphore_signal(barrier, inc=1, device_id={'w': lax.rem(me + off, group)}, device_id_type=MESH)

    def load_pair(g, start, size):
        own = pl.ds(start, size)
        return (pltpu.make_async_copy(coef_hbm.at[own], coef.at[own], load_sem.at[0, g]),
                pltpu.make_async_copy(leg_hbm.at[pl.ds(me * wave_loc + start, size)], leg.at[own], load_sem.at[1, g]))

    def load_block(b):
        gap = skip(b)
        return pltpu.make_async_copy(
            coef_hbm.at[pl.ds(BLOCK * (b % blocks), BLOCK), :, pl.ds(tri_m + gap, tri_deg - gap), :],
            tri.at[pl.ds(BLOCK * b, BLOCK), :, pl.ds(gap, tri_deg - gap), :], load_sem.at[b % blocks % 2, b % blocks // 2])

    @pl.when(is_full)
    def _():
        for args in starts(SIZES_A):
            for copy in load_pair(*args):
                copy.start()

    for b in range(CORES * blocks):
        @pl.when(me == full + b // blocks)
        def _():
            load_block(b).start()

    leg_tri_copy = pltpu.make_async_copy(leg_hbm.at[pl.ds(tri_m, tri_num), pl.ds(tri_m, tri_deg), :], leg_tri, mat_sem.at[2])
    mats = [leg_tri_copy, pltpu.make_async_copy(inv_hbm, inv, mat_sem.at[0]), pltpu.make_async_copy(fwd_hbm, fwd, mat_sem.at[1]),
            pltpu.make_async_copy(pick_early_hbm, pick_early, mat_sem.at[3]), pltpu.make_async_copy(pick_last_hbm, pick_last, mat_sem.at[4])]
    for copy in mats:
        copy.start()

    low = lax.broadcasted_iota(jnp.int32, (SUB, levels), 0) < QUAD

    def copy_a(off, c, start, size):
        dst = lax.rem(me + off, group)
        return pltpu.make_async_remote_copy(
            src_ref=send_a.at[rows((dst * chunks + c) * msg + start, size)],
            dst_ref=recv_a.at[rows((c * group + me) * msg + start, size)],
            send_sem=send_sem_a, recv_sem=recv_sem_a.at[c], device_id={'w': dst}, device_id_type=MESH)

    def copy_b(dst, c, start, size, sem):
        return pltpu.make_async_remote_copy(
            src_ref=send_b.at[rows((c * group + dst) * msg + start, size)],
            dst_ref=recv_b.at[rows((c * group + me) * msg + start, size)],
            send_sem=send_sem_b, recv_sem=sem, device_id={'w': dst}, device_id_type=MESH)

    def after_parts(dst, c):
        return jnp.logical_and(jnp.logical_and(chip == 1, dst < CORES), c >= HELD)

    def copy_relay(dst, c):
        slot = c * CORES + lax.rem(dst, CORES)
        return pltpu.make_async_remote_copy(
            src_ref=send_b.at[rows((c * group + dst) * msg, msg)], dst_ref=relay.at[rows(slot * msg, msg)],
            send_sem=send_sem_b, recv_sem=recv_sem_b.at[slot], device_id={'w': full + core}, device_id_type=MESH)

    def copy_onward(c, e):
        slot = c * CORES + e
        return pltpu.make_async_remote_copy(
            src_ref=relay.at[rows(slot * msg, msg)], dst_ref=recv_b.at[rows((c * group + core) * msg, msg)],
            send_sem=misc_send, recv_sem=recv_sem_b.at[c], device_id={'w': group // 2 + e}, device_id_type=MESH)

    def copy_tri(b, dst):
        gap = skip(b)
        ref = tri.at[pl.ds(BLOCK * b, BLOCK), :, pl.ds(gap, tri_deg - gap), :]
        return pltpu.make_async_remote_copy(
            src_ref=ref, dst_ref=ref, send_sem=misc_send, recv_sem=tri_recv.at[b],
            device_id={'w': dst}, device_id_type=MESH)

    def entry(b, at):
        return (b // CORES if at == 1 else b) % CORES

    def gets(b):
        return jnp.where(chip == 1, entry(b, 1), entry(b, 0)) == core

    def keeps(b):
        return jnp.where(is_tri, b // blocks, b % CORES) == core

    def mate_slot(b):
        return jnp.where(is_tri, b % blocks, b // CORES)

    def copy_mate(b):
        gap = skip(b)
        return pltpu.make_async_remote_copy(
            src_ref=part_own.at[pl.ds(BLOCK * b, BLOCK), :, pl.ds(gap, tri_deg - gap), :],
            dst_ref=part_mate.at[pl.ds(BLOCK * mate_slot(b), BLOCK), :, pl.ds(gap, tri_deg - gap), :],
            send_sem=misc_send, recv_sem=mate_recv.at[mate_slot(b)], device_id={'w': mate}, device_id_type=MESH)

    def copy_part(b):
        gap = skip(b)
        to_first = chip == 1
        slot = jnp.where(chip == chips - 2, 1, 0)
        dst = jnp.where(to_first, core, full + b // blocks)
        return pltpu.make_async_remote_copy(
            src_ref=part_own.at[pl.ds(BLOCK * b, BLOCK), :, pl.ds(gap, tri_deg - gap), :],
            dst_ref=part_in.at[slot, pl.ds(BLOCK * (b % blocks), BLOCK), :, pl.ds(gap, tri_deg - gap), :],
            send_sem=misc_send, recv_sem=part_recv.at[slot, b % blocks], device_id={'w': dst}, device_id_type=MESH)

    def wait_part(b, slot):
        gap = skip(b)
        landed = part_in.at[slot, pl.ds(BLOCK * (b % blocks), BLOCK), :, pl.ds(gap, tri_deg - gap), :]
        pltpu.make_async_copy(landed, landed, part_recv.at[slot, b % blocks]).wait()

    def wait_rows(ref, sem, count):
        landed = ref.at[pl.ds(0, count)]
        pltpu.make_async_copy(landed, landed, sem).wait()

    order = [group // 2, 2, group - 2, group // 2 + 1, 3, group - 1, 1]
    order = order if sorted(order) == list(range(1, group)) else list(range(1, group))

    def held(off, c):
        dst_chip = lax.div(lax.rem(me + off, group), CORES)
        return jnp.logical_and(jnp.logical_and(forwards, dst_chip == 1), c >= HELD)

    @pl.when(is_full)
    def _():
        for g, start, size in starts(SIZES_A):
            for copy in load_pair(g, start, size):
                copy.wait()

            def legendre_body(i, carry):
                m = start + i
                leg_hi, leg_lo = split(jnp.transpose(leg[m]))
                c_hi, c_lo = split(jnp.concatenate([coef[m, 0], coef[m, 1]], axis=1))
                f = dot(leg_hi, c_hi) + dot(leg_lo, c_hi) + dot(leg_hi, c_lo)
                for t in range(group * lat_loc // SUB):
                    re = f[t * SUB:(t + 1) * SUB, :levels]
                    im = f[t * SUB:(t + 1) * SUB, levels:]
                    send_a[rows((2 * t * wave_loc + m) * SUB, SUB), :] = jnp.where(low, re, pltpu.roll(im, QUAD, 0))
                    send_a[rows(((2 * t + 1) * wave_loc + m) * SUB, SUB), :] = jnp.where(low, pltpu.roll(re, QUAD, 0), im)
                return carry

            lax.fori_loop(0, size, legendre_body, 0, unroll=4)
            if g == 0:
                pl.semaphore_wait(barrier, group - 1)
            for off in order:
                copy_a(off, 0, start * SUB, size * SUB).start()
            if g < EARLY:
                for off in order:
                    @pl.when(jnp.logical_not(held(off, 1)))
                    def _():
                        copy_a(off, 1, start * SUB, size * SUB).start()

        rest = sum(SIZES_A[:EARLY])
        for off in order:
            @pl.when(jnp.logical_not(held(off, 1)))
            def _():
                copy_a(off, 1, rest * SUB, (wave_loc - rest) * SUB).start()

        @pl.loop(2, chunks)
        def _(c):
            for off in order:
                @pl.when(jnp.logical_not(held(off, c)))
                def _():
                    copy_a(off, c, 0, msg).start()

        @pl.loop(0, chunks)
        def _(c):
            recv_a[rows((c * group + me) * msg, msg), :] = send_a[rows((me * chunks + c) * msg, msg), :]

    @pl.when(is_tri)
    def _():
        pl.semaphore_wait(barrier, group - 1)
        for b in range(CORES * blocks):
            @pl.when(core == b // blocks)
            def _():
                load_block(b).wait()
                for dst in (full - CORES + entry(b, chips - 2), entry(b, 0), mate):
                    copy_tri(b, dst).start()

    @pl.when(forwards)
    def _():
        for b in range(CORES * blocks):
            @pl.when(gets(b))
            def _():
                copy_tri(b, mate).wait_recv()
                copy_tri(b, full - 2 * CORES + entry(b, 1)).start()
                copy_tri(b, mate).start()

        @pl.loop(1, chunks)
        def _(c):
            for off in order:
                @pl.when(held(off, c))
                def _():
                    copy_a(off, c, 0, msg).start()

    leg_tri_copy.wait()
    lat_all = group * lat_loc

    pick = lax.broadcasted_iota(jnp.int32, (lat_all, OWN), 0) == lax.broadcasted_iota(jnp.int32, (lat_all, OWN), 1) + me * lat_loc
    pick = jnp.logical_and(pick, lax.broadcasted_iota(jnp.int32, (lat_all, OWN), 1) < lat_loc)
    pick = jnp.where(pick, 1.0, 0.0).astype(BF16)

    def own_body(m, carry):
        for half, value in enumerate(split(leg_tri[m])):
            mine = dot(value, pick)
            leg_own_t[half, m] = mine.astype(BF16)
            leg_own[half, m] = jnp.transpose(mine).astype(BF16)
        return carry

    lax.fori_loop(0, tri_num, own_body, 0, unroll=4)

    for b in range(CORES * blocks):
        @pl.when(jnp.logical_and(jnp.logical_and(is_full, jnp.logical_not(forwards)), gets(b)))
        def _():
            copy_tri(b, mate).wait_recv()
            copy_tri(b, mate).start()

    for b in range(CORES * blocks):
        @pl.when(jnp.logical_not(jnp.where(is_tri, core == b // blocks, gets(b))))
        def _():
            copy_tri(b, mate).wait_recv()

    def tri_body(m, carry):
        own_hi, own_lo = leg_own[0, m], leg_own[1, m]
        c_hi, c_lo = split(jnp.concatenate([tri[m, 0], tri[m, 1]], axis=1))
        f = dot(own_hi, c_hi) + dot(own_lo, c_hi) + dot(own_hi, c_lo)
        for c in range(chunks):
            t = c // 2
            re = f[t * SUB:(t + 1) * SUB, :levels]
            im = f[t * SUB:(t + 1) * SUB, levels:]
            tile = jnp.where(low, pltpu.roll(re, QUAD, 0), im) if c % 2 else jnp.where(low, re, pltpu.roll(im, QUAD, 0))
            recv_a[rows(((c * group + full) * wave_loc + m) * SUB, SUB), :] = tile
        return carry

    lax.fori_loop(0, tri_num, tri_body, 0, unroll=4)

    for copy in mats[1:]:
        copy.wait()

    @pl.loop(0, chunks)
    def _(c):
        @pl.when(is_full)
        def _():
            wait_rows(recv_a, recv_sem_a.at[c], (full - 1) * msg)

        @pl.when(is_tri)
        def _():
            wait_rows(recv_a, recv_sem_a.at[c], full * msg)

        @pl.loop(0, QUAD // 2)
        def _(pair):
            halves = []
            for u in range(2):
                row = c * (group * msg) + 2 * pair + u
                re = recv_a[pl.ds(row, waves, stride=SUB), :]
                im = recv_a[pl.ds(row + QUAD, waves, stride=SUB), :]
                halves.append(jnp.concatenate([re, im], axis=0))
            f_hi, f_lo = split(jnp.concatenate(halves, axis=1))
            g_val = dot(inv[...], jnp.concatenate([f_hi, f_lo, f_hi], axis=0))
            for u in range(2):
                grid[c * QUAD + 2 * pair + u] = g_val[:, u * levels:(u + 1) * levels]
            q_hi, q_lo = split(g_val * g_val)
            h = dot(fwd[...], jnp.concatenate([q_hi, q_lo, q_hi], axis=0))
            for u in range(2):
                row = c * (group * msg) + 2 * pair + u
                hw = h[:, u * levels:(u + 1) * levels] * wt_ref[me * lat_loc + c * QUAD + 2 * pair + u]
                send_b[pl.ds(row, waves, stride=SUB), :] = hw[:waves]
                send_b[pl.ds(row + QUAD, waves, stride=SUB), :] = hw[waves:]

        @pl.when(c < chunks - 1)
        def _():
            for off in order:
                dst = lax.rem(me + off, group)
                by_relay = jnp.logical_and(jnp.logical_and(chip == 0, dst >= group // 2), c < RELAYED)

                @pl.when(jnp.logical_and(dst < full, by_relay))
                def _():
                    copy_relay(dst, c).start()

                late = jnp.logical_and(is_tri, lax.div(dst, CORES) == 1)

                ready = jnp.logical_and(jnp.logical_or(jnp.logical_not(late), c >= LAG), jnp.logical_not(after_parts(dst, c)))

                @pl.when(jnp.logical_and(jnp.logical_and(dst < full, jnp.logical_not(by_relay)), ready))
                def _():
                    copy_b(dst, c, 0, msg, recv_sem_b.at[c]).start()

                @pl.when(jnp.logical_and(late, c == LAG))
                def _():
                    for before in range(LAG):
                        copy_b(dst, before, 0, msg, recv_sem_b.at[before]).start()

        @pl.when(is_full)
        def _():
            recv_b[rows((c * group + me) * msg, msg), :] = send_b[rows((c * group + me) * msg, msg), :]

    zero = jnp.zeros((SUB, levels), F32)

    def part_body(i, carry):
        side = jnp.where(i < wave_loc, 1 - core, core)
        spread = BLOCK * (CORES * lax.div(lax.rem(i, wave_loc), BLOCK) + side) + lax.rem(i, BLOCK)
        m = jnp.where(is_tri, lax.rem(i, wave_loc) + side * wave_loc, spread)
        re, im = [], []
        for t in range(OWN // SUB):
            a, b = (send_b[rows((c * waves + tri_m + m) * SUB, SUB), :] if c < chunks else zero for c in (2 * t, 2 * t + 1))
            re.append(jnp.where(low, a, pltpu.roll(b, QUAD, 0)))
            im.append(jnp.where(low, pltpu.roll(a, QUAD, 0), b))
        h_hi, h_lo = split(jnp.concatenate([jnp.concatenate(re, axis=0), jnp.concatenate(im, axis=0)], axis=1))
        own_hi, own_lo = leg_own_t[0, m], leg_own_t[1, m]
        p_val = dot(own_hi, h_hi) + dot(own_lo, h_hi) + dot(own_hi, h_lo)
        part_own[m, 0] = p_val[:, :levels]
        part_own[m, 1] = p_val[:, levels:]
        return carry

    lax.fori_loop(0, wave_loc, part_body, 0, unroll=4)
    for b in range(CORES * blocks):
        @pl.when(jnp.logical_not(keeps(b)))
        def _():
            copy_mate(b).start()
    lax.fori_loop(wave_loc, tri_num, part_body, 0, unroll=4)
    for b in range(CORES * blocks):
        @pl.when(keeps(b))
        def _():
            copy_mate(b).wait_recv()

            @pl.loop(0, BLOCK)
            def _(i):
                gap = skip(b)
                for r in range(2):
                    part_own[BLOCK * b + i, r, gap:, :] += part_mate[BLOCK * mate_slot(b) + i, r, gap:, :]

        @pl.when(jnp.logical_and(jnp.logical_and(is_full, chip > 0), core == b % CORES))
        def _():
            copy_part(b).start()

    for c in range(chunks - 1):
        for off in order:
            dst = lax.rem(me + off, group)

            @pl.when(after_parts(dst, c))
            def _():
                copy_b(dst, c, 0, msg, recv_sem_b.at[c]).start()

    for off in order:
        dst = lax.rem(me + off, group)

        @pl.when(dst < full)
        def _():
            copy_b(dst, chunks - 1, 0, msg, recv_sem_b.at[chunks - 1]).start()

    @pl.when(is_full)
    def _():
        def pick_body(m, carry):
            leg_hi, leg_lo = split(leg[m])
            leg_early[m] = (dot(leg_hi, pick_early[0]) + dot(leg_lo, pick_early[1])).astype(BF16)
            leg_last[m] = (dot(leg_hi, pick_last[0]) + dot(leg_lo, pick_last[1])).astype(BF16)
            return carry

        lax.fori_loop(0, wave_loc, pick_body, 0, unroll=2)

    for b in range(CORES * blocks):
        @pl.when(jnp.logical_and(chip == 0, core == b % CORES))
        def _():
            gap = skip(b)
            wait_part(b, 0)

            @pl.loop(0, BLOCK)
            def _(i):
                for r in range(2):
                    part_own[BLOCK * b + i, r, gap:, :] += part_in[0, BLOCK * (b % blocks) + i, r, gap:, :]

            copy_part(b).start()

    @pl.when(is_tri)
    def _():
        for c in range(RELAYED):
            for e in range(CORES):
                slot = c * CORES + e
                landed = relay.at[pl.ds(slot * msg, msg)]
                pltpu.make_async_copy(landed, landed, recv_sem_b.at[slot]).wait()
                copy_onward(c, e).start()

    @pl.when(is_full)
    def _():
        for c in range(chunks - 2):
                wait_rows(recv_b, recv_sem_b.at[c], (group - 1) * msg)

        def early_body(m, carry):
            s_val = sums(recv_b, leg_early[m], m, range(chunks - 2), group, wave_loc, levels)
            for r in range(2):
                spec[m, r] = s_val[:, r * levels:(r + 1) * levels]
            return carry

        lax.fori_loop(0, wave_loc, early_body, 0, unroll=2)
        for c in range(chunks - 2, chunks):
            wait_rows(recv_b, recv_sem_b.at[c], (group - 1) * msg)

    for b in range(CORES * blocks):
        @pl.when(me == full + b // blocks)
        def _():
            gap = skip(b)
            for slot in range(2):
                wait_part(b, slot)

            @pl.loop(0, BLOCK)
            def _(i):
                m = BLOCK * (b % blocks) + i
                for r in range(2):
                    acc = part_own[BLOCK * b + i, r, gap:, :]
                    for slot in range(2):
                        acc = acc + part_in[slot, m, r, gap:, :]
                    spec[m, r, :tri_m + gap, :] = jnp.zeros((tri_m + gap, levels), F32)
                    spec[m, r, tri_m + gap:, :] = acc

    @pl.when(is_full)
    def _():
        wait_rows(send_a, send_sem_a, (group - 1) * chunks * msg)
        wait_rows(send_b, send_sem_b, (full - 1) * chunks * msg)

    @pl.when(is_tri)
    def _():
        wait_rows(send_b, send_sem_b, full * chunks * msg)

    def block_rows(blks):
        return sum(BLOCK * 2 * (tri_deg - skip(b)) for b in blks)

    for at in range(chips):
        for p in range(CORES):
            if at == chips - 1:
                own = [b for b in range(CORES * blocks) if b // blocks == p]
                mates = [b for b in range(CORES * blocks) if b // blocks != p]
                count = 3 * block_rows(own) + block_rows(mates) + RELAYED * CORES * msg
            else:
                come = [b for b in range(CORES * blocks) if entry(b, at) == p]
                count = block_rows(come) * (2 if at == chips - 2 else 1) + block_rows(range(CORES * blocks))

            @pl.when(jnp.logical_and(chip == at, core == p))
            def _():
                wait_rows(send_a, misc_send, count)


def finish(dims, grid, early, recv_b, leg_last, grid_hbm, spec_hbm, spec, grid_sem, spec_sem):
    group, wave_loc, levels, degs, lat_loc, waves, lon = dims
    chunks = lat_loc // QUAD
    is_full = lax.axis_index('w') < group - CORES
    copies = []
    for p in range(PIECES):
        part = pl.ds(p * (lat_loc // PIECES), lat_loc // PIECES)
        copies.append(pltpu.make_async_copy(grid.at[part], grid_hbm.at[part], grid_sem.at[p]))
        copies[-1].start()
    size = wave_loc // PIECES
    for p in range(PIECES):
        part = pl.ds(p * size, size)

        @pl.when(is_full)
        def _():
            def last_body(i, carry):
                m = p * size + i
                s_val = sums(recv_b, leg_last[m], m, (chunks - 2, chunks - 1), group, wave_loc, levels)
                for r in range(2):
                    spec[m, r] = early[m, r] + s_val[:, r * levels:(r + 1) * levels]
                return carry

            lax.fori_loop(0, size, last_body, 0, unroll=4)
            pltpu.make_async_copy(spec.at[part], spec_hbm.at[part], spec_sem.at[p]).start()

        @pl.when(jnp.logical_not(is_full))
        def _():
            pltpu.make_async_copy(early.at[part], spec_hbm.at[part], spec_sem.at[p]).start()

        copies.append(pltpu.make_async_copy(spec.at[part], spec_hbm.at[part], spec_sem.at[p]))
    for copy in copies:
        copy.wait()


def solution(mesh):
    group = mesh.shape['w']

    def per_device(coef, legendre, gauss_weight):
        wave_loc, _, levels, degs = coef.shape
        waves = wave_loc * group
        lon = 2 * waves
        lat_loc = legendre.shape[2] // group
        coef_t = jnp.transpose(coef, (0, 1, 3, 2))
        inv, fwd = (jnp.asarray(x) for x in fourier_matrices(waves))
        tri_num = CORES * wave_loc
        tri_deg = degs - waves + tri_num
        blocks = tri_num // BLOCK
        chunks = lat_loc // QUAD
        pick_early = jnp.asarray(latitude_picks(group, lat_loc, 0, chunks - 2))
        pick_last = jnp.asarray(latitude_picks(group, lat_loc, chunks - 2, 2))
        total = group * lat_loc // QUAD * wave_loc * SUB
        dims = (group, wave_loc, levels, degs, lat_loc, waves, lon)
        hbm = pl.BlockSpec(memory_space=pltpu.HBM)
        vmem = pl.BlockSpec(memory_space=pltpu.VMEM)
        dma = pltpu.SemaphoreType.DMA
        grid, spec, recv_b, leg_last = pl.pallas_call(
            functools.partial(kernel, dims),
            out_shape=(pltpu.VMEM((lat_loc, lon, levels), F32), pltpu.VMEM(coef_t.shape, F32), pltpu.VMEM((total, levels), F32), pltpu.VMEM((wave_loc, degs, pick_last.shape[2]), BF16)),
            in_specs=[hbm, hbm, hbm, hbm, hbm, hbm, pl.BlockSpec(memory_space=pltpu.SMEM)],
            out_specs=(vmem, vmem, vmem, vmem),
            scratch_shapes=[
                pltpu.VMEM(coef_t.shape, F32),
                pltpu.VMEM((wave_loc, degs, legendre.shape[2]), F32),
                pltpu.VMEM(inv.shape, BF16),
                pltpu.VMEM(fwd.shape, BF16),
                pltpu.VMEM((total, levels), F32),
                pltpu.VMEM((total, levels), F32),
                pltpu.VMEM((total, levels), F32),
                pltpu.VMEM((tri_num, 2, tri_deg, levels), F32),
                pltpu.VMEM((tri_num, tri_deg, legendre.shape[2]), F32),
                pltpu.VMEM((2, tri_num, OWN, tri_deg), BF16),
                pltpu.VMEM((2, tri_num, tri_deg, OWN), BF16),
                pltpu.VMEM((tri_num, 2, tri_deg, levels), F32),
                pltpu.VMEM((wave_loc, 2, tri_deg, levels), F32),
                pltpu.VMEM((2, wave_loc, 2, tri_deg, levels), F32),
                pltpu.VMEM((RELAYED * CORES * wave_loc * SUB, levels), F32),
                pltpu.VMEM(pick_early.shape, BF16),
                pltpu.VMEM(pick_last.shape, BF16),
                pltpu.VMEM((wave_loc, degs, pick_early.shape[2]), BF16),
                dma((2, len(SIZES_A))), dma((5,)), dma, dma((lat_loc // QUAD,)), dma, dma((lat_loc // QUAD,)),
                dma((blocks,)), dma((blocks // CORES,)), dma((2, blocks // CORES)), dma,
            ],
            compiler_params=pltpu.CompilerParams(collective_id=0, has_side_effects=True, vmem_limit_bytes=52 * 2**20),
            name='transform_pair',
        )(coef_t, legendre, inv, fwd, pick_early, pick_last, gauss_weight)
        grid, spec = pl.pallas_call(
            functools.partial(finish, dims),
            out_shape=(jax.ShapeDtypeStruct(grid.shape, F32), jax.ShapeDtypeStruct(spec.shape, F32)),
            in_specs=[vmem, vmem, vmem, vmem],
            out_specs=(hbm, hbm),
            scratch_shapes=[pltpu.VMEM(spec.shape, F32), dma((PIECES,)), dma((PIECES,))],
            compiler_params=pltpu.CompilerParams(vmem_limit_bytes=8 * 2**20),
            name='finish',
        )(grid, spec, recv_b, leg_last)
        return jnp.transpose(grid, (2, 0, 1)), jnp.transpose(spec, (0, 1, 3, 2))

    return jax.shard_map(per_device, mesh=mesh, in_specs=(P('w', None, 'lev', None), P(None, None, None), P(None)), out_specs=(P('lev', 'w', None), P('w', None, 'lev', None)), check_vma=False)
```
